16 devices in a mesh: tp: 4 (over z, y), cp: 4 (over x, core).
Axes of the slice: x: 2, y: 2, z: 2, core: 2. Of those that a mesh axis runs over, the one named last changes fastest.
Arguments:
- x_in: bfloat16 [32, 512, 3072], P(None, 'cp')
- grad_z: bfloat16 [32, 512, 3072], P(None, 'cp')
- seg_pos: int32 [32, 512], P(None, 'cp')
- norm_scale: bfloat16 [3072], replicated
- w_x: bfloat16 [3072, 3072], P(None, 'tp')
- b_x: bfloat16 [3072], P('tp')
- w_y: bfloat16 [3072, 3072], P(None, 'tp')
- b_y: bfloat16 [3072], P('tp')
- conv_w: bfloat16 [4, 3072], P(None, 'tp')
- conv_b: bfloat16 [3072], P('tp')
- w_a: bfloat16 [24, 128, 128], P('tp')
- b_a: bfloat16 [3072], P('tp')
- w_i: bfloat16 [24, 128, 128], P('tp')
- b_i: bfloat16 [3072], P('tp')
- a_param: float32 [3072], P('tp')
- w_out: bfloat16 [3072, 3072], P('tp')
- b_out: bfloat16 [3072], replicated
Outputs:
- output 1: bfloat16 [32, 512, 3072], P(None, 'cp')
- output 2: bfloat16 [32, 512, 3072], P(None, 'cp')
- output 3: float32 [3072], replicated
- output 4: float32 [3072, 3072], P(None, 'tp')
- output 5: float32 [3072], P('tp')
- output 6: float32 [3072, 3072], P(None, 'tp')
- output 7: float32 [3072], P('tp')
- output 8: float32 [4, 3072], P(None, 'tp')
- output 9: float32 [3072], P('tp')
- output 10: float32 [24, 128, 128], P('tp')
- output 11: float32 [3072], P('tp')
- output 12: float32 [24, 128, 128], P('tp')
- output 13: float32 [3072], P('tp')
- output 14: float32 [3072], P('tp')
- output 15: float32 [3072, 3072], P('tp')
- output 16: float32 [3072], replicated
All inputs are finite; a program needn't handle non-finite values.
Results may differ from the reference program's by a relative error of at most 0.00700116.
Values sent between devices are 32-bit elements.
A program may use at most 1 GiB of HBM per device.

```python
import math
import jax
import jax.numpy as jnp
from jax import lax

BATCH_SEQS = 32
SEQ_LEN = 512
D_MODEL = 3072
D_RNN = 3072
GATE_BLOCKS = 24
DOC_STARTS = 2
CONV_WIDTH = 4
BLOCK_WIDTH = D_RNN // GATE_BLOCKS
NORM_EPS = 1e-6


def doc_positions(pos_key):
    starts = jax.random.randint(pos_key, (BATCH_SEQS, DOC_STARTS), 1, SEQ_LEN)
    step_ids = jnp.arange(SEQ_LEN, dtype=jnp.int32)
    is_start = jnp.any(step_ids[None, :, None] == starts[:, None, :], axis=-1) | (step_ids == 0)[None, :]
    last_start = lax.cummax(jnp.where(is_start, step_ids[None, :], 0), axis=1)
    return (step_ids[None, :] - last_start).astype(jnp.int32)


def setup_inputs(seed: int = 0) -> dict:
    key_list = jax.random.split(jax.random.key(seed), 17)

    def draw_normal(key_index, arr_shape, factor):
        return jax.random.normal(key_list[key_index], arr_shape, jnp.float32) * factor

    tok_shape = (BATCH_SEQS, SEQ_LEN, D_MODEL)
    gate_shape = (GATE_BLOCKS, BLOCK_WIDTH, BLOCK_WIDTH)
    soft_plus = jnp.exp(jax.random.uniform(key_list[14], (D_RNN,), jnp.float32, math.log(2e-5), math.log(2e-4)))
    return {
        "x_in": draw_normal(0, tok_shape, 1.0).astype(jnp.bfloat16),
        "grad_z": draw_normal(1, tok_shape, 1.0).astype(jnp.bfloat16),
        "seg_pos": doc_positions(key_list[2]),
        "norm_scale": draw_normal(3, (D_MODEL,), 0.3).astype(jnp.bfloat16),
        "w_x": draw_normal(4, (D_MODEL, D_RNN), D_MODEL ** -0.5).astype(jnp.bfloat16),
        "b_x": draw_normal(5, (D_RNN,), 0.3).astype(jnp.bfloat16),
        "w_y": draw_normal(6, (D_MODEL, D_RNN), D_MODEL ** -0.5).astype(jnp.bfloat16),
        "b_y": draw_normal(7, (D_RNN,), 0.3).astype(jnp.bfloat16),
        "conv_w": draw_normal(8, (CONV_WIDTH, D_RNN), 0.5).astype(jnp.bfloat16),
        "conv_b": draw_normal(9, (D_RNN,), 0.3).astype(jnp.bfloat16),
        "w_a": draw_normal(10, gate_shape, BLOCK_WIDTH ** -0.5).astype(jnp.bfloat16),
        "b_a": draw_normal(11, (D_RNN,), 0.5).astype(jnp.bfloat16),
        "w_i": draw_normal(12, gate_shape, BLOCK_WIDTH ** -0.5).astype(jnp.bfloat16),
        "b_i": draw_normal(13, (D_RNN,), 0.5).astype(jnp.bfloat16),
        "a_param": jnp.log(jnp.expm1(soft_plus)),
        "w_out": draw_normal(15, (D_RNN, D_MODEL), D_RNN ** -0.5).astype(jnp.bfloat16),
        "b_out": draw_normal(16, (D_MODEL,), 0.3).astype(jnp.bfloat16),
    }


def to_bf16(arr_val):
    return arr_val + lax.stop_gradient(arr_val.astype(jnp.bfloat16).astype(jnp.float32) - arr_val)


def block_forward(x_f, norm_scale, w_x, b_x, w_y, b_y, conv_w, conv_b, w_a, b_a, w_i, b_i, a_param, w_out, b_out, seg_pos):
    mean_sq = jnp.mean(x_f * x_f, axis=-1, keepdims=True)
    normed = to_bf16(x_f * lax.rsqrt(mean_sq + NORM_EPS) * (1.0 + norm_scale))
    y_act = jax.nn.gelu(jnp.dot(normed, w_y, preferred_element_type=jnp.float32) + b_y, approximate=True)
    x_branch = to_bf16(jnp.dot(normed, w_x, preferred_element_type=jnp.float32) + b_x)
    batch_n, seq_n, width_n = x_branch.shape
    conv_sum = x_branch * conv_w[0] + conv_b
    for tap_k in range(1, CONV_WIDTH):
        shifted = jnp.pad(x_branch[:, :seq_n - tap_k], ((0, 0), (tap_k, 0), (0, 0)))
        keep_mask = (seg_pos >= tap_k)[:, :, None]
        conv_sum = conv_sum + jnp.where(keep_mask, shifted, 0.0) * conv_w[tap_k]
    conv_out = to_bf16(conv_sum)
    blocks = conv_out.reshape(batch_n, seq_n, GATE_BLOCKS, BLOCK_WIDTH)
    pre_a = jnp.einsum("bthk,hkj->bthj", blocks, w_a).reshape(batch_n, seq_n, width_n) + b_a
    pre_i = jnp.einsum("bthk,hkj->bthj", blocks, w_i).reshape(batch_n, seq_n, width_n) + b_i
    reset_mask = (seg_pos == 0)[:, :, None]
    log_a = -8.0 * jax.nn.sigmoid(pre_a) * jax.nn.softplus(a_param)
    decays = jnp.where(reset_mask, 0.0, jnp.exp(log_a))
    multiplier = jnp.where(reset_mask, 1.0, jnp.sqrt(-jnp.expm1(2.0 * log_a)))
    drives = multiplier * jax.nn.sigmoid(pre_i) * conv_out

    def scan_step(carry_h, inputs_t):
        next_h = inputs_t[0] * carry_h + inputs_t[1]
        return next_h, next_h

    init_h = jnp.zeros((batch_n, width_n), jnp.float32)
    _, hidden_t = lax.scan(scan_step, init_h, (jnp.swapaxes(decays, 0, 1), jnp.swapaxes(drives, 0, 1)))
    hidden = jnp.swapaxes(hidden_t, 0, 1)
    mixed_v = to_bf16(hidden * y_act)
    out_proj = jnp.dot(mixed_v, w_out, preferred_element_type=jnp.float32) + b_out
    return to_bf16(x_f + out_proj)


def reference(x_in, grad_z, seg_pos, norm_scale, w_x, b_x, w_y, b_y, conv_w, conv_b, w_a, b_a, w_i, b_i, a_param, w_out, b_out):
    primals = [param_arr.astype(jnp.float32) for param_arr in (x_in, norm_scale, w_x, b_x, w_y, b_y, conv_w, conv_b, w_a, b_a, w_i, b_i, a_param, w_out, b_out)]

    def run_block(*params):
        return block_forward(*params, seg_pos)

    z_val, pull_back = jax.vjp(run_block, *primals)
    grad_list = pull_back(grad_z.astype(jnp.float32))
    return (z_val.astype(jnp.bfloat16), grad_list[0].astype(jnp.bfloat16), grad_list[1], grad_list[2], grad_list[3], grad_list[4], grad_list[5], grad_list[6], grad_list[7], grad_list[8], grad_list[9], grad_list[10], grad_list[11], grad_list[12], grad_list[13], grad_list[14])
```

```python
import functools
import jax
import jax.numpy as jnp
from jax import lax
from jax.experimental import pallas as pl
from jax.experimental.pallas import tpu as pltpu
from jax.sharding import PartitionSpec as P

NORM_EPS = 1e-6
CONV_WIDTH = 4
HALO = CONV_WIDTH - 1
LANES = 128
CB = 256
TC = 16
TINY = 1.2e-38
GELU_A = 0.7978845608028654
GELU_B = 0.044715
VMEM_BYTES = 64 * 1024 * 1024 - 64 * 1024
F32 = jnp.float32
BF16 = jnp.bfloat16
IN_SPECS = (P(None, "cp", None), P(None, "cp", None), P(None, "cp"), P(), P(None, "tp"), P("tp"), P(None, "tp"), P("tp"), P(None, "tp"), P("tp"), P("tp", None, None), P("tp"), P("tp", None, None), P("tp"), P("tp"), P("tp", None), P())
OUT_SPECS = (P(None, "cp", None), P(None, "cp", None), P(), P(None, "tp"), P("tp"), P(None, "tp"), P("tp"), P(None, "tp"), P("tp"), P("tp", None, None), P("tp"), P("tp", None, None), P("tp"), P("tp"), P("tp", None), P())
R_BX, R_BY, R_CB, R_BA, R_BI, R_K, R_CW = 0, 1, 2, 3, 4, 5, 6
PAR_ROWS = 16


def dot_nn(lhs, rhs):
    return jnp.dot(lhs, rhs, preferred_element_type=F32)


def dot_nt(lhs, rhs):
    return lax.dot_general(lhs, rhs, (((1,), (1,)), ((), ())), preferred_element_type=F32)


def dot_tn(lhs, rhs):
    return lax.dot_general(lhs, rhs, (((0,), (0,)), ((), ())), preferred_element_type=F32)


def round16(val):
    return val.astype(BF16).astype(F32)


def sigmoid(val):
    return 1.0 / (1.0 + jnp.exp(-val))


def gates(pre_a, pre_i, slope, keep):
    gate_r = sigmoid(pre_a)
    gate_i = sigmoid(pre_i)
    log_a = gate_r * slope
    raw_a = jnp.exp(log_a)
    gap = jnp.tanh(-log_a) * (1.0 + raw_a * raw_a)
    inv_m = lax.rsqrt(jnp.maximum(gap, TINY))
    decay = jnp.where(keep, raw_a, 0.0)
    mult = jnp.where(keep, gap * inv_m, 1.0)
    return gate_r, gate_i, decay, mult, inv_m


def first_pass_kernel(ids_ref, n_ref, gz_ref, nh_ref, pos_ref, wx_ref, wy_ref, wo_ref, wg_ref, par_ref, *rest, n_blk, n_chunk, own, batch):
    if own:
        c_out, y_out, g_out, q_out, info_out, xb_out, xh, xs, ys, ds, pre, tail, state = rest
        wx_b, wy_b, wo_b = wx_ref, wy_ref, wo_ref
    else:
        c_out, y_out, g_out, q_out, info_out, wx_b, wy_b, wo_b, xs, ys, ds, pre, xh, tail, state = rest
        xb_out = None
    step = pl.program_id(0)
    n_steps = n_blk * n_chunk

    @pl.when((lax.rem(step, n_chunk) == 0) & (step < n_steps))
    def _():
        if not own:
            wx_b[...] = wx_ref[0].astype(BF16)
            wy_b[...] = wy_ref[0].astype(BF16)
            wo_b[...] = wo_ref[0].astype(BF16)
        xh[...] = dot_nn(nh_ref[...].astype(BF16), wx_b[...])

    def dots():
        rows = n_ref[...]
        xs[...] = dot_nn(rows, wx_b[...])
        ys[...] = dot_nn(rows, wy_b[...])
        ds[...] = dot_nt(gz_ref[...], wo_b[...])

    def elementwise():
        first = lax.rem(step + n_chunk - 1, n_chunk) == 0
        for half in range(CB // LANES):
            lane = slice(half * LANES, (half + 1) * LANES)
            row = lambda idx: par_ref[0, idx:idx + 1, lane]
            bias_x, conv_b = row(R_BX), row(R_CB)
            taps = [row(R_CW + k) for k in range(CONV_WIDTH)]
            past = []
            for j in range(HALO):
                sl = slice(j * batch, (j + 1) * batch)
                past.append(jnp.where(first, round16(xh[sl, lane] + bias_x), tail[sl, lane]))
            for t in range(TC):
                sl = slice(t * batch, (t + 1) * batch)
                cur = round16(xs[sl, lane] + bias_x)
                if own:
                    xb_out[0, t, :, lane] = cur.astype(BF16)
                pos = pos_ref[t]
                total = conv_b + cur * taps[0]
                for k in range(1, CONV_WIDTH):
                    total = total + jnp.where(pos >= k, past[HALO - k], 0.0) * taps[k]
                c_out[0, t, :, lane] = total.astype(BF16)
                past = past[1:] + [cur]
            for j in range(HALO):
                tail[j * batch:(j + 1) * batch, lane] = past[j]
            wg = wg_ref[0, half].astype(BF16)
            pre[half] = dot_nn(c_out[0, :, :, lane].reshape(TC * batch, LANES), wg)
            bias_y, bias_a, bias_i, slope = row(R_BY), row(R_BA), row(R_BI), row(R_K)
            hid = jnp.where(first, 0.0, state[0, :, lane])
            prod = jnp.where(first, 1.0, state[1, :, lane])
            head = jnp.where(first, 0.0, state[2, :, lane])
            for t in range(TC):
                sl = slice(t * batch, (t + 1) * batch)
                keep = pos_ref[t] >= 1
                conv = c_out[0, t, :, lane].astype(F32)
                _, gate_i, decay, mult, _ = gates(pre[half, sl, :LANES] + bias_a, pre[half, sl, LANES:] + bias_i, slope, keep)
                hid = decay * hid + mult * gate_i * conv
                prod = prod * decay
                pre_y = ys[sl, lane] + bias_y
                sq = pre_y * pre_y
                tan = jnp.tanh(pre_y * (GELU_A + GELU_A * GELU_B * sq))
                half_y = 0.5 * pre_y
                d_mixed = ds[sl, lane]
                y_act = half_y + half_y * tan
                slope_y = 0.5 + 0.5 * tan + half_y * (1.0 - tan * tan) * (GELU_A + 3.0 * GELU_A * GELU_B * sq)
                grad_h = d_mixed * y_act
                head = head + prod * grad_h
                y_out[0, t, :, lane] = y_act
                g_out[0, t, :, lane] = grad_h
                q_out[0, t, :, lane] = d_mixed * slope_y
            for idx, val in enumerate((hid, prod, head)):
                state[idx, :, lane] = val
                info_out[idx, :, lane] = val

    @pl.when(step == 0)
    def _():
        dots()

    @pl.when((step > 0) & (step < n_steps))
    def _():
        elementwise()
        dots()

    @pl.when(step == n_steps)
    def _():
        elementwise()


def first_pass(ids, normed, gz, n_halo, pos_b, wx, wy, wo, wg, par, own):
    n_blk = ids.shape[0]
    n_rows, width = normed.shape
    n_tok, batch = pos_b.shape[0], pos_b.shape[1]
    n_chunk = n_tok // TC
    n_steps = n_blk * n_chunk
    cols = n_blk * CB
    cur = lambda s: jnp.minimum(s, n_steps - 1)
    old = lambda s: jnp.maximum(s - 1, 0)
    row_spec = pl.BlockSpec((TC * batch, width), lambda s, ids: (lax.rem(cur(s), n_chunk), 0))
    if own:
        w_specs = [pl.BlockSpec((width, CB), lambda s, ids: (0, cur(s) // n_chunk))] * 2 + [pl.BlockSpec((CB, width), lambda s, ids: (cur(s) // n_chunk, 0))]
    else:
        w_specs = [pl.BlockSpec((1, width, CB), lambda s, ids: (ids[cur(s) // n_chunk], 0, 0))] * 2 + [pl.BlockSpec((1, CB, width), lambda s, ids: (ids[cur(s) // n_chunk], 0, 0))]
    in_specs = [row_spec, row_spec, pl.BlockSpec((HALO * batch, width), lambda s, ids: (0, 0)),
                pl.BlockSpec((TC, batch, LANES), lambda s, ids: (lax.rem(old(s), n_chunk), 0, 0)), *w_specs,
                pl.BlockSpec((1, CB // LANES, LANES, 2 * LANES), lambda s, ids: (ids[old(s) // n_chunk], 0, 0, 0)),
                pl.BlockSpec((1, PAR_ROWS, CB), lambda s, ids: (ids[old(s) // n_chunk], 0, 0))]
    tok_spec = pl.BlockSpec((1, TC, batch, CB), lambda s, ids: (old(s) // n_chunk, lax.rem(old(s), n_chunk), 0, 0))
    tok_shape = lambda dt: jax.ShapeDtypeStruct((n_blk, n_tok, batch, CB), dt)
    out_specs = [tok_spec] * 4 + [pl.BlockSpec((3, batch, CB), lambda s, ids: (0, 0, old(s) // n_chunk))]
    out_shape = [tok_shape(BF16), tok_shape(F32), tok_shape(F32), tok_shape(F32), jax.ShapeDtypeStruct((3, batch, cols), F32)]
    if own:
        out_specs += [tok_spec, pl.BlockSpec((HALO * batch, CB), lambda s, ids: (0, cur(s) // n_chunk))]
        out_shape += [tok_shape(BF16), jax.ShapeDtypeStruct((HALO * batch, cols), F32)]
    else:
        out_specs += [pl.BlockSpec((width, CB), lambda s, ids: (0, cur(s) // n_chunk))] * 2 + [pl.BlockSpec((CB, width), lambda s, ids: (cur(s) // n_chunk, 0))]
        out_shape += [jax.ShapeDtypeStruct((width, cols), BF16)] * 2 + [jax.ShapeDtypeStruct((cols, width), BF16)]
    rows = TC * batch
    scratch = [pltpu.VMEM((rows, CB), F32)] * 3 + [pltpu.VMEM((CB // LANES, rows, 2 * LANES), F32)] + [pltpu.VMEM((HALO * batch, CB), F32)] * (1 if own else 2) + [pltpu.VMEM((3, batch, CB), F32)]
    flops = 6 * n_rows * width * cols
    return pl.pallas_call(
        functools.partial(first_pass_kernel, n_blk=n_blk, n_chunk=n_chunk, own=own, batch=batch),
        grid_spec=pltpu.PrefetchScalarGridSpec(num_scalar_prefetch=1, grid=(n_steps + 1,), in_specs=in_specs, out_specs=out_specs, scratch_shapes=scratch),
        out_shape=out_shape,
        compiler_params=pltpu.CompilerParams(dimension_semantics=("arbitrary",), vmem_limit_bytes=VMEM_BYTES),
        cost_estimate=pl.CostEstimate(flops=flops, bytes_accessed=n_blk * n_rows * width * 4, transcendentals=0),
        name="first_pass_own" if own else "first_pass_far",
    )(ids, normed, gz, n_halo, pos_b, wx, wy, wo, wg, par)


N_ACC = 11


def second_pass_kernel(ids_ref, c_ref, y_ref, g_ref, q_ref, pos_ref, enter_ref, wg_ref, par_ref, *rest, n_chunk, own, batch):
    if own:
        xb_ref, xh_ref, mix_out, dpy_out, dbr_out, head_out, tail_out, acc_out, gw_out, s_a, s_A, s_i, s_m, pre, dpai, dgate, s_e = rest
    else:
        mix_out, dpy_out, dbr_out, head_out, tail_out, s_a, s_A, s_i, s_m, pre, dpai, dgate = rest
    row = lambda idx: par_ref[0, idx:idx + 1, :]
    wg = wg_ref[0, 0].astype(BF16)
    bias_a, bias_i, slope = row(R_BA), row(R_BI), row(R_K)
    taps = [row(R_CW + k) for k in range(CONV_WIDTH)]
    fold = lambda val: jnp.sum(val.reshape(batch // 8, 8, LANES), axis=0)
    if own:
        halo = [round16(xh_ref[k] + row(R_BX)) for k in range(HALO)]
        acc_out[...] = jnp.zeros_like(acc_out)
        gw_out[...] = jnp.zeros_like(gw_out)

    def forward(j, hid):
        base = j * TC
        pre[...] = dot_nn(c_ref[0, pl.ds(base, TC)].reshape(TC * batch, LANES), wg)
        acc_y = jnp.zeros((8, LANES), F32)
        for t in range(TC):
            sl = slice(t * batch, (t + 1) * batch)
            tok = base + t
            keep = pos_ref[tok] >= 1
            conv = c_ref[0, tok].astype(F32)
            gate_r, gate_i, decay, mult, inv_m = gates(pre[sl, :LANES] + bias_a, pre[sl, LANES:] + bias_i, slope, keep)
            in_conv = gate_i * conv
            before = hid
            hid = decay * before + mult * in_conv
            d_log = decay * (before - in_conv * decay * inv_m)
            r_log = d_log * gate_r
            s_a[tok] = decay
            s_A[tok] = r_log * (1.0 - gate_r) * slope
            s_i[tok] = mult * in_conv * (1.0 - gate_i)
            s_m[tok] = mult * gate_i
            mix_out[tok] = (hid * y_ref[0, tok]).astype(BF16)
            d_pre_y = hid * q_ref[0, tok]
            dpy_out[tok] = d_pre_y.astype(BF16)
            if own:
                s_e[tok] = r_log
                acc_y = acc_y + fold(d_pre_y)
        if own:
            acc_out[0, 8:16] = acc_out[0, 8:16] + acc_y
        return hid

    lax.fori_loop(0, n_chunk, forward, enter_ref[0])

    def recur(j, carry):
        base = j * TC
        acc_a = acc_i = acc_p = jnp.zeros((8, LANES), F32)
        for t in range(TC - 1, -1, -1):
            sl = slice(t * batch, (t + 1) * batch)
            tok = base + t
            grad_h = g_ref[0, tok] + carry
            carry = s_a[tok] * grad_h
            d_pre_a = grad_h * s_A[tok]
            d_pre_i = grad_h * s_i[tok]
            s_m[tok] = grad_h * s_m[tok]
            dpai[sl, :LANES] = d_pre_a.astype(BF16)
            dpai[sl, LANES:] = d_pre_i.astype(BF16)
            if own:
                acc_a = acc_a + fold(d_pre_a)
                acc_i = acc_i + fold(d_pre_i)
                acc_p = acc_p + fold(grad_h * s_e[tok])
        dgate[...] = dot_nt(dpai[...], wg)
        if own:
            acc_out[0, 16:24] = acc_out[0, 16:24] + acc_a
            acc_out[0, 24:32] = acc_out[0, 24:32] + acc_i
            acc_out[0, 32:40] = acc_out[0, 32:40] + acc_p
            gw_out[0] = gw_out[0] + dot_tn(c_ref[0, pl.ds(base, TC)].reshape(TC * batch, LANES), dpai[...])
        return carry

    def conv_back(j, later):
        base = j * TC
        later = list(later)
        acc_x = acc_b = jnp.zeros((8, LANES), F32)
        acc_w = [jnp.zeros((8, LANES), F32) for _ in range(CONV_WIDTH)]
        for t in range(TC - 1, -1, -1):
            sl = slice(t * batch, (t + 1) * batch)
            tok = base + t
            d_conv = s_m[tok] + dgate[sl]
            total = d_conv * taps[0] + later[0]
            pos = pos_ref[tok]
            masked = [jnp.where(pos >= k, d_conv, 0.0) for k in range(1, CONV_WIDTH)]
            later = [later[1] + masked[0] * taps[1], later[2] + masked[1] * taps[2], masked[2] * taps[3]]
            dbr_out[tok] = total.astype(BF16)
            if t >= TC - HALO:
                tail_out[t - (TC - HALO)] = jnp.where(j == n_chunk - 1, total, tail_out[t - (TC - HALO)])
            if own:
                acc_x = acc_x + fold(total)
                acc_b = acc_b + fold(d_conv)
                acc_w[0] = acc_w[0] + fold(d_conv * xb_ref[0, tok].astype(F32))
                for k in range(1, CONV_WIDTH):
                    past = xb_ref[0, jnp.maximum(tok - k, 0)].astype(F32)
                    if t < k:
                        past = jnp.where(j == 0, halo[HALO + t - k], past)
                    acc_w[k] = acc_w[k] + fold(masked[k - 1] * past)
        if own:
            acc_out[0, 0:8] = acc_out[0, 0:8] + acc_x
            acc_out[0, 40:48] = acc_out[0, 40:48] + acc_b
            for k in range(CONV_WIDTH):
                acc_out[0, 48 + 8 * k:56 + 8 * k] = acc_out[0, 48 + 8 * k:56 + 8 * k] + acc_w[k]
        return tuple(later)

    tail_out[...] = jnp.zeros_like(tail_out)
    zero = jnp.zeros((batch, LANES), F32)
    carry = recur(n_chunk - 1, enter_ref[1])

    def back(idx, vals):
        carry, later = vals[0], vals[1:]
        j = n_chunk - 2 - idx
        later = conv_back(j + 1, later)
        carry = recur(j, carry)
        return (carry, *later)

    vals = lax.fori_loop(0, n_chunk - 1, back, (carry, zero, zero, zero))
    later = conv_back(0, vals[1:])
    for k in range(HALO):
        head_out[HALO - 1 - k] = later[k]


def second_pass(ids, conv, y_act, grad_h, q_val, pos_b, enter, wg, par, xb=None, xb_halo=None):
    own = xb is not None
    n_blk, n_tok, batch, _ = conv.shape
    n_chunk = n_tok // TC
    per = CB // LANES
    cols = n_blk * CB
    tok_spec = pl.BlockSpec((1, n_tok, batch, LANES), lambda s, ids: (s // per, 0, 0, lax.rem(s, per)))
    lane_spec = lambda n: pl.BlockSpec((n, batch, LANES), lambda s, ids: (0, 0, s))
    in_specs = [tok_spec] * 4 + [pl.BlockSpec((n_tok, batch, LANES), lambda s, ids: (0, 0, 0)), lane_spec(2),
                pl.BlockSpec((1, 1, LANES, 2 * LANES), lambda s, ids: (ids[s // per], lax.rem(s, per), 0, 0)),
                pl.BlockSpec((1, PAR_ROWS, LANES), lambda s, ids: (ids[s // per], 0, lax.rem(s, per)))]
    out_specs = [lane_spec(n_tok)] * 3 + [lane_spec(HALO)] * 2
    out_shape = [jax.ShapeDtypeStruct((n_tok, batch, cols), BF16)] * 3 + [jax.ShapeDtypeStruct((HALO, batch, cols), F32)] * 2
    scratch = [pltpu.VMEM((n_tok, batch, LANES), F32)] * 4 + [pltpu.VMEM((TC * batch, 2 * LANES), F32), pltpu.VMEM((TC * batch, 2 * LANES), BF16), pltpu.VMEM((TC * batch, LANES), F32)]
    args = [ids, conv, y_act, grad_h, q_val, pos_b, enter, wg, par]
    if own:
        in_specs += [tok_spec, lane_spec(HALO)]
        out_specs += [pl.BlockSpec((1, 8 * N_ACC - 8, LANES), lambda s, ids: (s, 0, 0)), pl.BlockSpec((1, LANES, 2 * LANES), lambda s, ids: (s, 0, 0))]
        out_shape += [jax.ShapeDtypeStruct((n_blk * per, 8 * N_ACC - 8, LANES), F32), jax.ShapeDtypeStruct((n_blk * per, LANES, 2 * LANES), F32)]
        scratch.append(pltpu.VMEM((n_tok, batch, LANES), F32))
        args += [xb, xb_halo]
    n_elem = n_tok * batch * cols
    return pl.pallas_call(
        functools.partial(second_pass_kernel, n_chunk=n_chunk, own=own, batch=batch),
        grid_spec=pltpu.PrefetchScalarGridSpec(num_scalar_prefetch=1, grid=(n_blk * per,), in_specs=in_specs, out_specs=out_specs, scratch_shapes=scratch),
        out_shape=out_shape,
        compiler_params=pltpu.CompilerParams(dimension_semantics=("arbitrary",), vmem_limit_bytes=VMEM_BYTES),
        cost_estimate=pl.CostEstimate(flops=n_elem * 12000, bytes_accessed=n_elem * 20, transcendentals=n_elem * 6),
        name="second_pass_own" if own else "second_pass_far",
    )(*args)


def out_kernel(mo_ref, mf_ref, wo_ref, wf_ref, x_ref, b_ref, z_ref):
    n_t, n_b, _ = mo_ref.shape
    proj = dot_nn(mo_ref[...].reshape(n_t * n_b, -1), wo_ref[...]) + dot_nn(mf_ref[...].reshape(n_t * n_b, -1), wf_ref[...])
    proj = jnp.swapaxes(proj.reshape(n_t, n_b, -1), 0, 1)
    z_ref[...] = (x_ref[...].astype(F32) + (proj + b_ref[...].reshape(1, 1, -1))).astype(BF16)


def out_pass(mix_own, mix_far, w_own, w_far, x_in, b_out):
    n_tok, batch, c_own = mix_own.shape
    c_far = mix_far.shape[2]
    width = x_in.shape[2]
    b_blk = 16
    act = lambda c: pl.BlockSpec((TC, b_blk, c), lambda i, j: (i, j, 0))
    full = lambda shape: pl.BlockSpec(shape, lambda i, j: (0,) * len(shape), pipeline_mode=pl.Buffered(1))
    native = pl.BlockSpec((b_blk, TC, width), lambda i, j: (j, i, 0))
    return pl.pallas_call(
        out_kernel, grid=(n_tok // TC, batch // b_blk),
        in_specs=[act(c_own), act(c_far), full(w_own.shape), full(w_far.shape), native, full((1, width))],
        out_specs=native, out_shape=jax.ShapeDtypeStruct(x_in.shape, BF16),
        compiler_params=pltpu.CompilerParams(dimension_semantics=("arbitrary", "arbitrary"), vmem_limit_bytes=VMEM_BYTES),
        cost_estimate=pl.CostEstimate(flops=2 * n_tok * batch * (c_own + c_far) * width, bytes_accessed=n_tok * batch * width * 8, transcendentals=0),
        name="out_pass",
    )(mix_own, mix_far, w_own, w_far, x_in, b_out)


def norm_back_kernel(do_ref, df_ref, po_ref, pf_ref, xo_ref, xf_ref, yo_ref, yf_ref, x_ref, gz_ref, s_ref, gx_ref, gs_ref):
    n_t, n_b, _ = do_ref.shape
    flat = lambda ref: ref[...].reshape(n_t * n_b, -1)
    d_n = dot_nt(flat(do_ref), xo_ref[...]) + dot_nt(flat(df_ref), xf_ref[...]) + dot_nt(flat(po_ref), yo_ref[...]) + dot_nt(flat(pf_ref), yf_ref[...])
    d_n = jnp.swapaxes(d_n.reshape(n_t, n_b, -1), 0, 1)
    x_f = x_ref[...].astype(F32)
    inv = lax.rsqrt(jnp.mean(x_f * x_f, axis=-1, keepdims=True) + NORM_EPS)
    x_hat = x_f * inv
    gain = 1.0 + s_ref[...].reshape(1, 1, -1)
    scaled = d_n * gain
    proj = jnp.mean(scaled * x_hat, axis=-1, keepdims=True)
    gx_ref[...] = (gz_ref[...].astype(F32) + inv * (scaled - x_hat * proj)).astype(BF16)
    part = jnp.sum((d_n * x_hat).reshape(n_t * n_b // 8, 8, -1), axis=0)

    @pl.when((pl.program_id(0) == 0) & (pl.program_id(1) == 0))
    def _():
        gs_ref[...] = jnp.zeros_like(gs_ref)
    gs_ref[...] += part


def norm_back_pass(dbr_own, dbr_far, dpy_own, dpy_far, wx_own, wx_far, wy_own, wy_far, x_in, grad_z, scale):
    n_tok, batch, c_own = dbr_own.shape
    c_far = dbr_far.shape[2]
    width = x_in.shape[2]
    b_blk = 16
    act = lambda c: pl.BlockSpec((TC, b_blk, c), lambda i, j: (i, j, 0))
    full = lambda shape: pl.BlockSpec(shape, lambda i, j: (0,) * len(shape), pipeline_mode=pl.Buffered(1))
    native = pl.BlockSpec((b_blk, TC, width), lambda i, j: (j, i, 0))
    return pl.pallas_call(
        norm_back_kernel, grid=(n_tok // TC, batch // b_blk),
        in_specs=[act(c_own), act(c_far), act(c_own), act(c_far), full(wx_own.shape), full(wx_far.shape), full(wy_own.shape), full(wy_far.shape), native, native, full((1, width))],
        out_specs=[native, full((8, width))],
        out_shape=[jax.ShapeDtypeStruct(x_in.shape, BF16), jax.ShapeDtypeStruct((8, width), F32)],
        compiler_params=pltpu.CompilerParams(dimension_semantics=("arbitrary", "arbitrary"), vmem_limit_bytes=VMEM_BYTES),
        cost_estimate=pl.CostEstimate(flops=4 * n_tok * batch * (c_own + c_far) * width, bytes_accessed=n_tok * batch * width * 10, transcendentals=0),
        name="norm_back_pass",
    )(dbr_own, dbr_far, dpy_own, dpy_far, wx_own, wx_far, wy_own, wy_far, x_in, grad_z, scale)


def entering(info, cp_index, swap_core, swap_x):
    end, prod, head = info[0], info[1], info[2]
    other = lax.ppermute(info, "cp", swap_core)
    o_end, o_prod, o_head = other[0], other[1], other[2]
    upper_core = cp_index % 2 == 1
    upper_chip = cp_index >= 2
    chip_end = jnp.where(upper_core, prod * o_end + end, o_prod * end + o_end)
    chip_head = jnp.where(upper_core, o_head + o_prod * head, head + prod * o_head)
    got = lax.ppermute(jnp.where(upper_chip, chip_head, chip_end), "cp", swap_x)
    from_low = jnp.where(upper_chip, got, 0.0)
    from_high = jnp.where(upper_chip, 0.0, got)
    state_in = jnp.where(upper_core, o_prod * from_low + o_end, from_low)
    grad_in = jnp.where(upper_core, from_high, o_head + o_prod * from_high)
    return jnp.stack([state_in, grad_in])


def shard_body(x_in, grad_z, seg_pos, norm_scale, w_x, b_x, w_y, b_y, conv_w, conv_b, w_a, b_a, w_i, b_i, a_param, w_out, b_out, fwd_perm, back_perm, cp_size, tp_size):
    cp_index = lax.axis_index("cp")
    tp_index = lax.axis_index("tp")
    batch, n_tok, width = x_in.shape
    c_own = w_x.shape[1]
    n_own = c_own // CB
    swap_core = [(j, j ^ 1) for j in range(cp_size)]
    swap_x = [(j, j ^ 2) for j in range(cp_size)]

    def spread(arr):
        n = arr.shape[0] // cp_size
        part = lax.dynamic_slice_in_dim(arr, cp_index * n, n, 0).astype(F32)
        return lax.all_gather(part, ("tp", "cp")).reshape(tp_size, *arr.shape)

    slope = -8.0 * jax.nn.softplus(a_param)
    rows = [b_x, b_y, conv_b, b_a, b_i, slope, *[conv_w[k] for k in range(CONV_WIDTH)]]
    par = jnp.stack([r.astype(F32) for r in rows] + [jnp.zeros_like(slope)] * (PAR_ROWS - len(rows)))
    par = par.reshape(PAR_ROWS, n_own, CB).transpose(1, 0, 2)
    wg = jnp.concatenate([w_a, w_i], axis=-1)
    par_all = lax.all_gather(par, "tp")
    wg_all = spread(wg.reshape(-1, 2 * LANES)).reshape(tp_size, n_own, CB // LANES, LANES, 2 * LANES)
    wg = wg.reshape(n_own, CB // LANES, LANES, 2 * LANES)
    parts = []
    for p in range(n_own):
        parts.append((spread(w_x[:, p * CB:(p + 1) * CB]), spread(w_y[:, p * CB:(p + 1) * CB]), spread(w_out[p * CB:(p + 1) * CB])))

    x_f = x_in.astype(F32)
    inv = lax.rsqrt(jnp.mean(x_f * x_f, axis=-1, keepdims=True) + NORM_EPS)
    normed = (x_f * inv * (1.0 + norm_scale.astype(F32))).astype(BF16).transpose(1, 0, 2)
    gz_t = grad_z.transpose(1, 0, 2)
    n_halo = lax.ppermute(normed[n_tok - HALO:].astype(F32), "cp", fwd_perm).reshape(HALO * batch, width)
    normed = normed.reshape(n_tok * batch, width)
    gz_t = gz_t.reshape(n_tok * batch, width)
    pos_b = jnp.broadcast_to(seg_pos.T[:, :, None], (n_tok, batch, LANES))

    own_ids = jnp.arange(n_own, dtype=jnp.int32)
    c_o, y_o, g_o, q_o, info_o, xb_o, xh_o = first_pass(own_ids, normed, gz_t, n_halo, pos_b, w_x, w_y, w_out, wg, par, True)
    enter_o = entering(info_o, cp_index, swap_core, swap_x)
    mix_o, dpy_o, dbr_o, head_o, tail_o, acc, g_gate = second_pass(own_ids, c_o, y_o, g_o, q_o, pos_b, enter_o, wg, par, xb_o, xh_o.reshape(HALO, batch, c_own))
    back_o = lax.ppermute(head_o, "cp", back_perm)
    dbr_o = dbr_o.at[n_tok - HALO:].set((tail_o + back_o).astype(BF16))

    far = jnp.stack([tp_index ^ k for k in range(1, tp_size)]).astype(jnp.int32)
    mixes, dpys, dbrs, wxs, wys, wos = [], [], [], [], [], []
    for p, (wx_p, wy_p, wo_p) in enumerate(parts):
        wg_p, par_p = wg_all[:, p], par_all[:, p]
        c_f, y_f, g_f, q_f, info_f, wx16, wy16, wo16 = first_pass(far, normed, gz_t, n_halo, pos_b, wx_p, wy_p, wo_p, wg_p, par_p, False)
        enter_f = entering(info_f, cp_index, swap_core, swap_x)
        mix_f, dpy_f, dbr_f, head_f, tail_f = second_pass(far, c_f, y_f, g_f, q_f, pos_b, enter_f, wg_p, par_p)
        back_f = lax.ppermute(head_f, "cp", back_perm)
        dbr_f = dbr_f.at[n_tok - HALO:].set((tail_f + back_f).astype(BF16))
        for lst, val in zip((mixes, dpys, dbrs, wxs, wys, wos), (mix_f, dpy_f, dbr_f, wx16, wy16, wo16)):
            lst.append(val)
    mix_f, dpy_f, dbr_f = [jnp.concatenate(v, axis=2) for v in (mixes, dpys, dbrs)]
    wx_f, wy_f, wo_f = jnp.concatenate(wxs, axis=1), jnp.concatenate(wys, axis=1), jnp.concatenate(wos, axis=0)
    z_out = out_pass(mix_o, mix_f, w_out, wo_f, x_in, b_out.astype(F32).reshape(1, width))
    grad_x, gs_part = norm_back_pass(dbr_o, dbr_f, dpy_o, dpy_f, w_x, wx_f, w_y, wy_f, x_in, grad_z, norm_scale.astype(F32).reshape(1, width))

    flat = lambda arr: arr.reshape(n_tok * batch, -1)
    g_w_x = dot_tn(normed, flat(dbr_o))
    g_w_y = dot_tn(normed, flat(dpy_o))
    g_w_out = dot_tn(flat(mix_o), gz_t)
    acc = acc.reshape(c_own // LANES, N_ACC - 1, 8, LANES).sum(axis=2).transpose(1, 0, 2).reshape(N_ACC - 1, c_own)
    g_b_x = acc[0] + jnp.sum(back_o, axis=(0, 1))
    g_a_param = -8.0 * jax.nn.sigmoid(a_param) * acc[4]
    g_b_out = jnp.sum(gz_t, axis=0, dtype=F32)
    g_scale = jnp.sum(gs_part, axis=0)
    sums = lax.psum((g_scale, g_w_x, g_b_x, g_w_y, acc[1], acc[6:10], acc[5], g_gate[:, :, :LANES], acc[2], g_gate[:, :, LANES:], acc[3], g_a_param, g_w_out, g_b_out), "cp")
    return (z_out, grad_x) + tuple(sums)


def solution(mesh):
    cp_size = mesh.shape["cp"]
    fwd_perm = [(j, j + 1) for j in range(cp_size - 1)]
    back_perm = [(j + 1, j) for j in range(cp_size - 1)]
    per_device = functools.partial(shard_body, fwd_perm=fwd_perm, back_perm=back_perm, cp_size=cp_size, tp_size=mesh.shape["tp"])
    return jax.shard_map(per_device, mesh=mesh, in_specs=IN_SPECS, out_specs=OUT_SPECS, check_vma=False)
```

```python
import functools
import jax
import jax.numpy as jnp
from jax import lax
from jax.experimental import pallas as pl
from jax.experimental.pallas import tpu as pltpu
from jax.sharding import PartitionSpec as P

NORM_EPS = 1e-6
CONV_WIDTH = 4
HALO = CONV_WIDTH - 1
LANES = 128
CB = 256
TC = 16
TINY = 1.2e-38
GELU_A = 0.7978845608028654
GELU_B = 0.044715
VMEM_BYTES = 67043328
F32 = jnp.float32
BF16 = jnp.bfloat16
TOKENS, COLS, CHANNEL = P(None, "cp"), P(None, "tp"), P("tp")
PARAM_SPECS = (P(), COLS, CHANNEL, COLS, CHANNEL, COLS, CHANNEL, CHANNEL, CHANNEL, CHANNEL, CHANNEL, CHANNEL, CHANNEL, P())
IN_SPECS = (TOKENS, TOKENS, TOKENS, *PARAM_SPECS)
OUT_SPECS = (TOKENS, TOKENS, *PARAM_SPECS)
R_BX, R_BY, R_CB, R_BA, R_BI, R_K, R_CW = range(7)
PAR_ROWS = 16
EXT_ROWS = 48
EXT_PAR = 256
N_TILE = 512
SUB = 8
B_BLK = 16


def dot_nn(lhs, rhs):
    return jnp.dot(lhs, rhs, preferred_element_type=F32)


def dot_nt(lhs, rhs):
    return lax.dot_general(lhs, rhs, (((1,), (1,)), ((), ())), preferred_element_type=F32)


def dot_tn(lhs, rhs):
    return lax.dot_general(lhs, rhs, (((0,), (0,)), ((), ())), preferred_element_type=F32)


def round16(val):
    return val.astype(BF16).astype(F32)


def sigmoid(val):
    return 1.0 / (1.0 + jnp.exp(-val))


def gates(pre_a, pre_i, slope, keep):
    gate_r = sigmoid(pre_a)
    gate_i = sigmoid(pre_i)
    log_a = gate_r * slope
    raw_a = jnp.exp(log_a)
    gap = jnp.tanh(-log_a) * (1.0 + raw_a * raw_a)
    inv_m = lax.rsqrt(jnp.maximum(gap, TINY))
    decay = jnp.where(keep, raw_a, 0.0)
    mult = jnp.where(keep, gap * inv_m, 1.0)
    return gate_r, gate_i, decay, mult, inv_m


def first_pass_kernel(n_ref, gz_ref, nh_ref, pos_ref, *rest, n_blk, n_chunk, own, batch):
    if own:
        ext, rest = rest[0], rest[1:]
        w_hbm, rest = rest[:3], rest[3:]
        c_out, y_out, g_out, q_out, info_out, xb_out, xh, w16, wo16, w_sem, xs, ys, ds, pre, tail, state = rest
    else:
        w_hbm, rest = rest[:4 * n_blk], rest[4 * n_blk:]
        c_out, y_out, g_out, q_out, info_out, ext, w_out, w16, stage, w_sem, o_sem, xs, ys, ds, pre, xh, tail, state = rest
        xb_out = None
    step = pl.program_id(0)
    width = n_ref.shape[1]
    quarter = width // 4

    def own_loads(blk):
        cols = pl.ds(blk * CB, CB)
        pair = [pltpu.make_async_copy(w_hbm[k].at[:, cols], w16.at[blk, k], w_sem.at[blk, k]) for k in range(2)]
        return pair + [pltpu.make_async_copy(w_hbm[2].at[cols, :], wo16.at[blk], w_sem.at[blk, 2])]

    def far_load(idx):
        return pltpu.make_async_copy(w_hbm[idx], stage.at[idx % 4], w_sem.at[idx])

    def stores(blk):
        return [pltpu.make_async_copy(w16.at[blk, k], w_out.at[k, :, pl.ds(blk * CB, CB)], o_sem.at[blk, k]) for k in range(3)]

    def dots(blk):
        rows = n_ref[:]
        xs[blk] = dot_nn(rows, w16[blk, 0])
        ys[blk] = dot_nn(rows, w16[blk, 1])
        ds[blk] = dot_nt(gz_ref[:], wo16[blk]) if own else dot_nn(gz_ref[:], w16[blk, 2])

    def fetch(blk):
        if own:
            for copy in own_loads(blk):
                copy.wait()
        else:
            core = lax.rem(lax.axis_index("cp"), 2)
            for i in range(4):
                far_load(4 * blk + i).wait()
                side = core if i < 2 else 1 - core
                start = pl.multiple_of((2 * side + i % 2) * quarter, quarter)
                for k in range(3):
                    w16[blk, k, pl.ds(start, quarter), :] = stage[i, k, :quarter].astype(BF16)
                    if i < 2:
                        ext[blk, (3 * i + k) * EXT_ROWS:(3 * i + k + 1) * EXT_ROWS] = stage[i, k, quarter:]
                if blk + 1 < n_blk:
                    far_load(4 * blk + 4 + i).start()
            for copy in stores(blk):
                copy.start()
        xh[blk] = dot_nn(nh_ref[:].astype(BF16), w16[blk, 0])

    def elementwise(blk):
        first = step == 1
        for half in range(CB // LANES):
            lane = slice(half * LANES, (half + 1) * LANES)
            row = lambda idx: ext[blk, EXT_PAR + idx:EXT_PAR + idx + 1, lane]
            bias_x, conv_b = row(R_BX), row(R_CB)
            taps = [row(R_CW + k) for k in range(CONV_WIDTH)]
            past = []
            for j in range(HALO):
                sl = slice(j * batch, (j + 1) * batch)
                past.append(jnp.where(first, round16(xh[blk, sl, lane] + bias_x), tail[blk, sl, lane]))
            for t in range(TC):
                sl = slice(t * batch, (t + 1) * batch)
                cur = round16(xs[blk, sl, lane] + bias_x)
                if own:
                    xb_out[blk, t, :, lane] = cur.astype(BF16)
                pos = pos_ref[t]
                total = conv_b + cur * taps[0]
                for k in range(1, CONV_WIDTH):
                    total = total + jnp.where(pos >= k, past[HALO - k], 0.0) * taps[k]
                c_out[blk, t, :, lane] = total.astype(BF16)
                past = past[1:] + [cur]
            for j in range(HALO):
                tail[blk, j * batch:(j + 1) * batch, lane] = past[j]
            wg = ext[blk, half * LANES:(half + 1) * LANES].astype(BF16)
            pre[half] = dot_nn(c_out[blk, :, :, lane].reshape(TC * batch, LANES), wg)
            bias_y, bias_a, bias_i, slope = row(R_BY), row(R_BA), row(R_BI), row(R_K)
            hid = jnp.where(first, 0.0, state[blk, 0, :, lane])
            prod = jnp.where(first, 1.0, state[blk, 1, :, lane])
            head = jnp.where(first, 0.0, state[blk, 2, :, lane])
            for t in range(TC):
                sl = slice(t * batch, (t + 1) * batch)
                keep = pos_ref[t] >= 1
                conv = c_out[blk, t, :, lane].astype(F32)
                _, gate_i, decay, mult, _ = gates(pre[half, sl, :LANES] + bias_a, pre[half, sl, LANES:] + bias_i, slope, keep)
                hid = decay * hid + mult * gate_i * conv
                prod = prod * decay
                pre_y = ys[blk, sl, lane] + bias_y
                sq = pre_y * pre_y
                tan = jnp.tanh(pre_y * (GELU_A + GELU_A * GELU_B * sq))
                half_y = 0.5 * pre_y
                d_mixed = ds[blk, sl, lane]
                y_act = half_y + half_y * tan
                slope_y = 0.5 + 0.5 * tan + half_y * (1.0 - tan * tan) * (GELU_A + 3.0 * GELU_A * GELU_B * sq)
                grad_h = d_mixed * y_act
                head = head + prod * grad_h
                y_out[blk, t, :, lane] = y_act
                g_out[blk, t, :, lane] = grad_h
                q_out[blk, t, :, lane] = d_mixed * slope_y
            for idx, val in enumerate((hid, prod, head)):
                state[blk, idx, :, lane] = val
                info_out[blk, idx, :, lane] = val

    @pl.when(step == 0)
    def _():
        if own:
            for blk in range(n_blk):
                for copy in own_loads(blk):
                    copy.start()
        else:
            for i in range(4):
                far_load(i).start()
        for blk in range(n_blk):
            fetch(blk)
            dots(blk)

    @pl.when((step > 0) & (step < n_chunk))
    def _():
        for blk in range(n_blk):
            elementwise(blk)
            dots(blk)

    @pl.when(step == n_chunk)
    def _():
        def last(blk, _):
            elementwise(blk)
            return 0

        lax.fori_loop(0, n_blk, last, 0)
        if not own:
            for blk in range(n_blk):
                for copy in stores(blk):
                    copy.wait()


def first_pass(n_blk, normed, gz, n_halo, pos_b, weights, ext=None):
    own = ext is not None
    n_rows, width = normed.shape
    n_tok, batch = pos_b.shape[0], pos_b.shape[1]
    n_chunk = n_tok // TC
    cols = n_blk * CB
    rows = TC * batch
    cur = lambda s: jnp.minimum(s, n_chunk - 1)
    old = lambda s: jnp.maximum(s - 1, 0)
    const = lambda shape: pl.BlockSpec(shape, lambda s: (0,) * len(shape))
    row_spec = pl.BlockSpec((rows, width), lambda s: (cur(s), 0))
    any_spec = pl.BlockSpec(memory_space=pl.ANY)
    in_specs = [row_spec, row_spec, const((HALO * batch, width)), pl.BlockSpec((TC, batch, LANES), lambda s: (old(s), 0, 0))]
    tok_spec = pl.BlockSpec((n_blk, TC, batch, CB), lambda s: (0, old(s), 0, 0))
    tok_shape = lambda dt: jax.ShapeDtypeStruct((n_blk, n_tok, batch, CB), dt)
    ext_shape = (n_blk, 6 * EXT_ROWS, CB)
    out_specs = [tok_spec] * 4 + [const((n_blk, 3, batch, CB))]
    out_shape = [tok_shape(BF16), tok_shape(F32), tok_shape(F32), tok_shape(F32), jax.ShapeDtypeStruct((n_blk, 3, batch, CB), F32)]
    work = [pltpu.VMEM((n_blk, rows, CB), F32)] * 3 + [pltpu.VMEM((CB // LANES, rows, 2 * LANES), F32)]
    halo = pltpu.VMEM((n_blk, HALO * batch, CB), F32)
    state = pltpu.VMEM((n_blk, 3, batch, CB), F32)
    args = [normed, gz, n_halo, pos_b]
    if own:
        in_specs.append(const(ext_shape))
        args.append(ext)
        out_specs += [tok_spec, const((n_blk, HALO * batch, CB))]
        out_shape += [tok_shape(BF16), jax.ShapeDtypeStruct((n_blk, HALO * batch, CB), F32)]
        scratch = [pltpu.VMEM((n_blk, 2, width, CB), BF16), pltpu.VMEM((n_blk, CB, width), BF16), pltpu.SemaphoreType.DMA((n_blk, 3)), *work, halo, state]
    else:
        out_specs += [const(ext_shape), any_spec]
        out_shape += [jax.ShapeDtypeStruct(ext_shape, F32), jax.ShapeDtypeStruct((3, width, cols), BF16)]
        scratch = [pltpu.VMEM((n_blk, 3, width, CB), BF16), pltpu.VMEM((4, *weights[0].shape), F32), pltpu.SemaphoreType.DMA((4 * n_blk,)), pltpu.SemaphoreType.DMA((n_blk, 3)), *work, halo, halo, state]
    in_specs += [any_spec] * len(weights)
    flops = 6 * n_rows * width * cols
    return pl.pallas_call(
        functools.partial(first_pass_kernel, n_blk=n_blk, n_chunk=n_chunk, own=own, batch=batch),
        grid=(n_chunk + 1,), in_specs=in_specs, out_specs=out_specs, scratch_shapes=scratch, out_shape=out_shape,
        compiler_params=pltpu.CompilerParams(dimension_semantics=("arbitrary",), vmem_limit_bytes=VMEM_BYTES),
        cost_estimate=pl.CostEstimate(flops=flops, bytes_accessed=n_rows * width * 4, transcendentals=0),
        name="first_pass_own" if own else "first_pass_far",
    )(*args, *weights)


def turned(val):
    return jnp.swapaxes(val, 0, 1)


def lane_tiles(width):
    return [slice(k, k + LANES) for k in range(0, width, LANES)]


def pre_kernel(x_ref, gz_ref, s_ref, n_out, gz_out, inv_out, gb_out):
    width = x_ref.shape[2]
    total = 0.0
    for lane in lane_tiles(width):
        x_f = x_ref[:, :, lane].astype(F32)
        total = total + x_f * x_f
    inv_out[:] = jnp.broadcast_to(lax.rsqrt(jnp.sum(total, axis=-1, keepdims=True) * (1.0 / width) + NORM_EPS), inv_out.shape)

    @pl.when(pl.program_id(0) == 0)
    def _():
        gb_out[:] = jnp.zeros_like(gb_out)

    for lane in lane_tiles(width):
        normed = x_ref[:, :, lane].astype(F32) * inv_out[:] * (1.0 + s_ref[:, lane])
        n_out[:, :, lane] = turned(normed).astype(BF16)
        gz_f = gz_ref[:, :, lane].astype(F32)
        gz_out[:, :, lane] = turned(gz_f).astype(BF16)
        gb_out[:, lane] += jnp.sum(gz_f.reshape(-1, SUB, LANES), axis=0)


def row_specs(batch, n_tok):
    per = batch // B_BLK
    n_steps = (n_tok // TC) * per
    cur = lambda s: jnp.minimum(s, n_steps - 1)
    old = lambda s: jnp.maximum(s - 1, 0)
    act = lambda lanes: pl.BlockSpec((TC, B_BLK, lanes), lambda s: (cur(s) // per, lax.rem(cur(s), per), 0))
    native = lambda lag, lanes: pl.BlockSpec((B_BLK, TC, lanes), lambda s: (lax.rem(lag(s), per), lag(s) // per, 0))
    return n_steps, cur, old, act, native


def pre_pass(x_in, grad_z, scale):
    batch, n_tok, width = x_in.shape
    n_steps, cur, _, act, native = row_specs(batch, n_tok)
    const = lambda shape: pl.BlockSpec(shape, lambda s: (0,) * len(shape))
    return pl.pallas_call(
        pre_kernel, grid=(n_steps,),
        in_specs=[native(cur, width), native(cur, width), const((1, width))], out_specs=[act(width), act(width), native(cur, LANES), const((SUB, width))],
        out_shape=[jax.ShapeDtypeStruct((n_tok, batch, width), BF16)] * 2 + [jax.ShapeDtypeStruct((batch, n_tok, LANES), F32), jax.ShapeDtypeStruct((SUB, width), F32)],
        compiler_params=pltpu.CompilerParams(dimension_semantics=("arbitrary",), vmem_limit_bytes=VMEM_BYTES),
        cost_estimate=pl.CostEstimate(flops=n_tok * batch * width * 200, bytes_accessed=n_tok * batch * width * 8, transcendentals=0),
        name="pre_pass",
    )(x_in, grad_z, scale)


def send_kernel(core_ref, wx_ref, wy_ref, wo_ref, ext_ref, *outs):
    quarter = wx_ref.shape[0]
    for idx, out in enumerate(outs):
        @pl.when(pl.program_id(0) == idx)
        def _():
            values = wx_ref[:].astype(F32), wy_ref[:].astype(F32), wo_ref[:].astype(F32).T
            for k, val in enumerate(values):
                out[k, :quarter] = val
                out[k, quarter:] = ext_ref[0, k * EXT_ROWS:(k + 1) * EXT_ROWS]


def send_pass(core, w_x, w_y, w_out, ext):
    (width, _), n_own = w_x.shape, len(ext)
    quarter = width // 4
    tall = pl.BlockSpec((quarter, CB), lambda i, core: (2 * core[0] + lax.rem(i, 2), i // 2))
    wide = pl.BlockSpec((CB, quarter), lambda i, core: (i // 2, 2 * core[0] + lax.rem(i, 2)))
    shape = (3, quarter + EXT_ROWS, CB)
    return pl.pallas_call(
        send_kernel,
        grid_spec=pltpu.PrefetchScalarGridSpec(num_scalar_prefetch=1, grid=(2 * n_own,), in_specs=[tall, tall, wide, pl.BlockSpec((1, 3 * EXT_ROWS, CB), lambda i, core: (i // 2, lax.rem(i, 2), 0))],
                                               out_specs=[pl.BlockSpec(shape, lambda i, core: (0, 0, 0))] * (2 * n_own)),
        out_shape=[jax.ShapeDtypeStruct(shape, F32)] * (2 * n_own),
        compiler_params=pltpu.CompilerParams(dimension_semantics=("arbitrary",), vmem_limit_bytes=VMEM_BYTES),
        cost_estimate=pl.CostEstimate(flops=10 ** 9, bytes_accessed=2 * 10 ** 7, transcendentals=0),
        name="send_pass",
    )(core, w_x, w_y, w_out, ext)


N_ACC = 10
ACC_ROWS = 8 * N_ACC


def second_pass_kernel(c_ref, y_ref, g_ref, q_ref, pos_ref, enter_ref, wg_ref, par_ref, *rest, n_chunk, own, batch):
    if own:
        xb_ref, xh_ref, mix_out, dpy_out, dbr_out, head_out, tail_out, acc_out, gw_out, s_a, s_A, s_i, s_m, pre, dpai, dgate, s_e = rest
    else:
        mix_out, dpy_out, dbr_out, head_out, tail_out, s_a, s_A, s_i, s_m, pre, dpai, dgate = rest
    row = lambda idx: par_ref[0, idx:idx + 1, :]
    wg = wg_ref[0].astype(BF16)
    enter = (enter_ref[0, 0], enter_ref[0, 1])
    bias_a, bias_i, slope = row(R_BA), row(R_BI), row(R_K)
    taps = [row(R_CW + k) for k in range(CONV_WIDTH)]

    def add(idx, val):
        acc_out[0, pl.ds(8 * idx, 8)] = acc_out[0, pl.ds(8 * idx, 8)] + val

    fold = lambda val: jnp.sum(val.reshape(batch // 8, 8, LANES), axis=0)
    if own:
        halo = [round16(xh_ref[0, k * batch:(k + 1) * batch] + row(R_BX)) for k in range(HALO)]
        acc_out[:] = jnp.zeros_like(acc_out)
        gw_out[:] = jnp.zeros_like(gw_out)

    def chunk_of(j):
        return c_ref[0, pl.ds(j * TC, TC)].reshape(TC * batch, LANES)

    def pre_gates(j):
        pre[:] = dot_nn(chunk_of(j), wg)

    def forward(j, hid):
        base = j * TC
        acc_y = jnp.zeros((8, LANES), F32)
        for t in range(TC):
            sl = slice(t * batch, (t + 1) * batch)
            tok = base + t
            keep = pos_ref[tok] >= 1
            conv = c_ref[0, tok].astype(F32)
            gate_r, gate_i, decay, mult, inv_m = gates(pre[sl, :LANES] + bias_a, pre[sl, LANES:] + bias_i, slope, keep)
            in_conv = gate_i * conv
            before = hid
            hid = decay * before + mult * in_conv
            d_log = decay * (before - in_conv * decay * inv_m)
            r_log = d_log * gate_r
            s_a[tok] = decay
            s_A[tok] = r_log * (1.0 - gate_r) * slope
            s_i[tok] = mult * in_conv * (1.0 - gate_i)
            s_m[tok] = mult * gate_i
            mix_out[tok] = (hid * y_ref[0, tok]).astype(BF16)
            d_pre_y = hid * q_ref[0, tok]
            dpy_out[tok] = d_pre_y.astype(BF16)
            if own:
                s_e[tok] = r_log
                acc_y = acc_y + fold(d_pre_y)
        if own:
            add(1, acc_y)
        pre_gates(jnp.minimum(j + 1, n_chunk - 1))
        return hid

    pre_gates(0)
    lax.fori_loop(0, n_chunk, forward, enter[0])

    def recur(j, carry):
        base = j * TC
        acc_a = acc_i = acc_p = jnp.zeros((8, LANES), F32)
        for t in range(TC - 1, -1, -1):
            sl = slice(t * batch, (t + 1) * batch)
            tok = base + t
            grad_h = g_ref[0, tok] + carry
            carry = s_a[tok] * grad_h
            d_pre_a = grad_h * s_A[tok]
            d_pre_i = grad_h * s_i[tok]
            s_m[tok] = grad_h * s_m[tok]
            dpai[sl, :LANES] = d_pre_a.astype(BF16)
            dpai[sl, LANES:] = d_pre_i.astype(BF16)
            if own:
                acc_a = acc_a + fold(d_pre_a)
                acc_i = acc_i + fold(d_pre_i)
                acc_p = acc_p + fold(grad_h * s_e[tok])
        if own:
            add(2, acc_a)
            add(3, acc_i)
            add(4, acc_p)
            gw_out[0] = gw_out[0] + dot_tn(chunk_of(j), dpai[:])
        return carry

    def conv_back(j, later):
        base = j * TC
        later = list(later)
        acc_x = acc_b = jnp.zeros((8, LANES), F32)
        acc_w = [jnp.zeros((8, LANES), F32) for _ in range(CONV_WIDTH)]
        for t in range(TC - 1, -1, -1):
            sl = slice(t * batch, (t + 1) * batch)
            tok = base + t
            d_conv = s_m[tok] + dgate[sl]
            total = d_conv * taps[0] + later[0]
            pos = pos_ref[tok]
            masked = [jnp.where(pos >= k, d_conv, 0.0) for k in range(1, CONV_WIDTH)]
            later = [later[1] + masked[0] * taps[1], later[2] + masked[1] * taps[2], masked[2] * taps[3]]
            dbr_out[tok] = total.astype(BF16)
            if t >= TC - HALO:
                tail_out[t - (TC - HALO)] = jnp.where(j == n_chunk - 1, total, tail_out[t - (TC - HALO)])
            if own:
                acc_x = acc_x + fold(total)
                acc_b = acc_b + fold(d_conv)
                acc_w[0] = acc_w[0] + fold(d_conv * xb_ref[0, tok].astype(F32))
                for k in range(1, CONV_WIDTH):
                    past = xb_ref[0, jnp.maximum(tok - k, 0)].astype(F32)
                    if t < k:
                        past = jnp.where(j == 0, halo[HALO + t - k], past)
                    acc_w[k] = acc_w[k] + fold(masked[k - 1] * past)
        if own:
            add(0, acc_x)
            add(5, acc_b)
            for k in range(CONV_WIDTH):
                add(6 + k, acc_w[k])
        return tuple(later)

    tail_out[:] = jnp.zeros_like(tail_out)
    zero = jnp.zeros((batch, LANES), F32)
    carry = recur(n_chunk - 1, enter[1])
    dgate[:] = dot_nt(dpai[:], wg)

    def back(idx, vals):
        carry, later = vals[0], vals[1:]
        j = n_chunk - 2 - idx
        carry = recur(j, carry)
        later = conv_back(j + 1, later)
        dgate[:] = dot_nt(dpai[:], wg)
        return (carry, *later)

    vals = lax.fori_loop(0, n_chunk - 1, back, (carry, zero, zero, zero))
    later = conv_back(0, vals[1:])
    for k in range(HALO):
        head_out[HALO - 1 - k] = later[k]


def second_pass(conv, y_act, grad_h, q_val, pos_b, enter, ext, xb=None, xb_halo=None):
    own = xb is not None
    n_blk, n_tok, batch, _ = conv.shape
    n_chunk = n_tok // TC
    per = CB // LANES
    cols = n_blk * CB
    tok_spec = pl.BlockSpec((1, n_tok, batch, LANES), lambda s: (s // per, 0, 0, lax.rem(s, per)))
    lane_spec = lambda n: pl.BlockSpec((n, batch, LANES), lambda s: (0, 0, s))
    in_specs = [tok_spec] * 4 + [pl.BlockSpec((n_tok, batch, LANES), lambda s: (0, 0, 0)),
                pl.BlockSpec((1, 2, batch, LANES), lambda s: (s // per, 0, 0, lax.rem(s, per))),
                pl.BlockSpec((1, LANES, CB), lambda s: (s // per, lax.rem(s, per), 0)),
                pl.BlockSpec((1, PAR_ROWS, LANES), lambda s: (s // per, EXT_PAR // PAR_ROWS, lax.rem(s, per)))]
    out_specs = [lane_spec(n_tok)] * 3 + [lane_spec(HALO)] * 2
    out_shape = [jax.ShapeDtypeStruct((n_tok, batch, cols), BF16)] * 3 + [jax.ShapeDtypeStruct((HALO, batch, cols), F32)] * 2
    scratch = [pltpu.VMEM((n_tok, batch, LANES), F32)] * 4 + [pltpu.VMEM((TC * batch, 2 * LANES), F32), pltpu.VMEM((TC * batch, 2 * LANES), BF16), pltpu.VMEM((TC * batch, LANES), F32)]
    args = [conv, y_act, grad_h, q_val, pos_b, enter, ext, ext]
    if own:
        in_specs += [tok_spec, pl.BlockSpec((1, HALO * batch, LANES), lambda s: (s // per, 0, lax.rem(s, per)))]
        out_specs += [pl.BlockSpec((1, ACC_ROWS, LANES), lambda s: (s, 0, 0)), pl.BlockSpec((1, LANES, 2 * LANES), lambda s: (s, 0, 0))]
        out_shape += [jax.ShapeDtypeStruct((n_blk * per, ACC_ROWS, LANES), F32), jax.ShapeDtypeStruct((n_blk * per, LANES, 2 * LANES), F32)]
        scratch.append(pltpu.VMEM((n_tok, batch, LANES), F32))
        args += [xb, xb_halo]
    n_elem = n_tok * batch * cols
    return pl.pallas_call(
        functools.partial(second_pass_kernel, n_chunk=n_chunk, own=own, batch=batch),
        grid=(n_blk * per,), in_specs=in_specs, out_specs=out_specs, scratch_shapes=scratch, out_shape=out_shape,
        compiler_params=pltpu.CompilerParams(dimension_semantics=("arbitrary",), vmem_limit_bytes=VMEM_BYTES),
        cost_estimate=pl.CostEstimate(flops=n_elem * 12000, bytes_accessed=n_elem * 20, transcendentals=n_elem * 6),
        name="second_pass_own" if own else "second_pass_far",
    )(*args)


def tile_of(j):
    return pl.ds(pl.multiple_of(j * N_TILE, N_TILE), N_TILE)


def out_kernel(*refs, n_part, n_steps, n_pass):
    mixes, refs = refs[:n_part], refs[n_part:]
    w_hbm, refs = refs[:n_part], refs[n_part:]
    pass_in, refs = refs[:n_pass], refs[n_pass:]
    x_ref, b_ref, z_ref, refs = refs[0], refs[1], refs[2], refs[3:]
    pass_out, refs = refs[:n_pass], refs[n_pass:]
    w_v, acc, sem = refs[:n_part], refs[n_part], refs[n_part + 1]
    rows = TC * B_BLK
    n_tiles = z_ref.shape[2] // N_TILE
    step = pl.program_id(0)

    def copies(j):
        tile = tile_of(j)
        first = pltpu.make_async_copy(w_hbm[0].at[:, tile], w_v[0].at[:, tile], sem.at[j, 0])
        return [first] + [pltpu.make_async_copy(w_hbm[i].at[2, tile, :], w_v[i].at[tile, :], sem.at[j, i]) for i in range(1, n_part)]

    def product(tile):
        proj = dot_nn(mixes[0][:].reshape(rows, -1), w_v[0][:, tile])
        for i in range(1, n_part):
            proj = proj + dot_nt(mixes[i][:].reshape(rows, -1), w_v[i][tile, :])
        acc[:, tile] = proj

    def finish():
        for lane in lane_tiles(z_ref.shape[2]):
            proj = turned(acc[:, lane].reshape(TC, B_BLK, LANES))
            z_ref[:, :, lane] = (x_ref[:, :, lane].astype(F32) + (proj + b_ref[:, lane])).astype(BF16)
        for src, dst in zip(pass_in, pass_out):
            dst[:] = src[:]

    @pl.when(step == 0)
    def _():
        for j in range(n_tiles):
            for copy in copies(j):
                copy.start()

        def first(j, _):
            for copy in copies(j):
                copy.wait()
            product(tile_of(j))
            return 0

        lax.fori_loop(0, n_tiles, first, 0)

    @pl.when((step > 0) & (step < n_steps))
    def _():
        finish()
        product(slice(None))

    @pl.when(step == n_steps)
    def _():
        finish()


def out_pass(mixes, w_own, w_far, x_in, b_out, sums):
    n_tok, batch, _ = mixes[0].shape
    width = x_in.shape[2]
    n_steps, _, old, act, native = row_specs(batch, n_tok)
    n_part = len(mixes)
    any_spec = pl.BlockSpec(memory_space=pl.ANY)
    strips = [pl.BlockSpec((g.shape[0] // n_steps, g.shape[1]), lambda s: (old(s), 0)) for g in sums]
    return pl.pallas_call(
        functools.partial(out_kernel, n_part=n_part, n_steps=n_steps, n_pass=len(sums)), grid=(n_steps + 1,),
        in_specs=[act(m.shape[2]) for m in mixes] + [any_spec] * n_part + strips + [native(old, width), pl.BlockSpec((1, width), lambda s: (0, 0))],
        out_specs=[native(old, width)] + strips, out_shape=[jax.ShapeDtypeStruct(a.shape, a.dtype) for a in (x_in, *sums)],
        scratch_shapes=[pltpu.VMEM(w_own.shape, BF16)] + [pltpu.VMEM(w.shape[1:], BF16) for w in w_far] + [pltpu.VMEM((TC * B_BLK, width), F32), pltpu.SemaphoreType.DMA((width // N_TILE, n_part))],
        compiler_params=pltpu.CompilerParams(dimension_semantics=("arbitrary",), vmem_limit_bytes=VMEM_BYTES),
        cost_estimate=pl.CostEstimate(flops=2 * n_tok * batch * width * width, bytes_accessed=n_tok * batch * width * 8, transcendentals=0),
        name="out_pass",
    )(*mixes, w_own, *w_far, *sums, x_in, b_out)


def norm_back_kernel(*refs, n_part, n_steps):
    n_all = 2 * n_part
    lhs, refs = refs[:n_all], refs[n_all:]
    w_hbm, refs = refs[:n_part + 1], refs[n_part + 1:]
    x_ref, inv_ref, gz_ref, s_ref, gx_ref, gs_ref, *refs = refs
    w_v, (acc, d_n, x_old, sums, scale, shift, sem) = refs[:n_all], refs[n_all:]
    rows = TC * B_BLK
    width = gx_ref.shape[2]
    n_tiles = width // N_TILE
    wide = width // 2
    step = pl.program_id(0)

    def copies(j):
        tile = tile_of(j)
        lst = []
        for k in range(2):
            for i in range(n_part):
                src = w_hbm[k].at[tile, :] if i == 0 else w_hbm[i + 1].at[k, tile, :]
                idx = k * n_part + i
                lst.append(pltpu.make_async_copy(src, w_v[idx].at[tile, :], sem.at[j, idx]))
        return lst

    def product(tile):
        val = dot_nt(lhs[0][:].reshape(rows, -1), w_v[0][tile, :])
        for arr, weight in zip(lhs[1:], w_v[1:]):
            val = val + dot_nt(arr[:].reshape(rows, -1), weight[tile, :])
        acc[:, tile] = val

    def turn(tiles):
        for lane in tiles:
            val = turned(acc[:, lane].reshape(TC, B_BLK, LANES))
            d_n[:, :, lane] = val
            x_t = x_ref[:, :, lane]
            x_old[:, :, lane] = x_t
            sums[:] += val * (1.0 + s_ref[:, lane]) * x_t.astype(F32)

    def close():
        inv = inv_ref[:]
        scale[:] = inv
        shift[:] = inv * inv * inv * (jnp.sum(sums[:], axis=-1, keepdims=True) * (1.0 / width))
        sums[:] = jnp.zeros_like(sums)

    def finish():
        for lane in lane_tiles(width):
            val, inv = d_n[:, :, lane], scale[:]
            x_f = x_old[:, :, lane].astype(F32)
            gx_ref[:, :, lane] = (gz_ref[:, :, lane].astype(F32) + (inv * (val * (1.0 + s_ref[:, lane])) - x_f * shift[:])).astype(BF16)
            gs_ref[:, lane] += jnp.sum((val * x_f * inv).reshape(-1, SUB, LANES), axis=0)

    low, high = lane_tiles(width)[:wide // LANES], lane_tiles(width)[wide // LANES:]

    @pl.when(step == 0)
    def _():
        gs_ref[:] = jnp.zeros_like(gs_ref)
        sums[:] = jnp.zeros_like(sums)
        for j in range(n_tiles):
            for copy in copies(j):
                copy.start()

        def first(j, _):
            for copy in copies(j):
                copy.wait()
            product(tile_of(j))
            return 0

        lax.fori_loop(0, n_tiles, first, 0)
        turn(low + high)
        close()

    @pl.when((step > 0) & (step < n_steps))
    def _():
        finish()
        product(slice(wide))
        turn(low)
        product(slice(wide, None))
        turn(high)
        close()

    @pl.when(step == n_steps)
    def _():
        finish()


def norm_back_pass(dbrs, dpys, wx_own, wy_own, w_far, x_in, inv_b, grad_z, scale):
    n_tok, batch, _ = dbrs[0].shape
    width = x_in.shape[2]
    n_steps, cur, old, act, native = row_specs(batch, n_tok)
    n_part = len(dbrs)
    const = lambda shape: pl.BlockSpec(shape, lambda s: (0,) * len(shape))
    planes = [pltpu.VMEM(wx_own.shape, BF16)] + [pltpu.VMEM(w.shape[1:], BF16) for w in w_far]
    block = lambda dt, lanes: pltpu.VMEM((B_BLK, TC, lanes), dt)
    return pl.pallas_call(
        functools.partial(norm_back_kernel, n_part=n_part, n_steps=n_steps), grid=(n_steps + 1,),
        in_specs=[act(m.shape[2]) for m in (*dbrs, *dpys)] + [pl.BlockSpec(memory_space=pl.ANY)] * (n_part + 1) + [native(cur, width), native(cur, LANES), native(old, width), const((1, width))],
        out_specs=[native(old, width), const((SUB, width))],
        out_shape=[jax.ShapeDtypeStruct(x_in.shape, BF16), jax.ShapeDtypeStruct((SUB, width), F32)],
        scratch_shapes=[*planes, *planes, pltpu.VMEM((TC * B_BLK, width), F32), block(F32, width), block(BF16, width), *[block(F32, LANES)] * 3, pltpu.SemaphoreType.DMA((width // N_TILE, 2 * n_part))],
        compiler_params=pltpu.CompilerParams(dimension_semantics=("arbitrary",), vmem_limit_bytes=VMEM_BYTES),
        cost_estimate=pl.CostEstimate(flops=4 * n_tok * batch * width * width, bytes_accessed=n_tok * batch * width * 10, transcendentals=0),
        name="norm_back_pass",
    )(*dbrs, *dpys, wx_own, wy_own, *w_far, x_in, inv_b, grad_z, scale)


def after(val, *deps):
    return lax.optimization_barrier((val, *deps))[0]


def entering(info, cp_index, swap_core, swap_x):
    end, prod, head = [info[:, k] for k in range(3)]
    other = lax.ppermute(info, "cp", swap_core)
    o_end, o_prod, o_head = [other[:, k] for k in range(3)]
    upper_core = cp_index % 2 == 1
    upper_chip = cp_index >= 2
    chip_end = jnp.where(upper_core, prod * o_end + end, o_prod * end + o_end)
    chip_head = jnp.where(upper_core, o_head + o_prod * head, head + prod * o_head)
    got = lax.ppermute(jnp.where(upper_chip, chip_head, chip_end), "cp", swap_x)
    from_low = jnp.where(upper_chip, got, 0.0)
    from_high = jnp.where(upper_chip, 0.0, got)
    state_in = jnp.where(upper_core, o_prod * from_low + o_end, from_low)
    grad_in = jnp.where(upper_core, from_high, o_head + o_prod * from_high)
    return jnp.stack([state_in, grad_in], axis=1)


def shard_body(x_in, grad_z, seg_pos, norm_scale, w_x, b_x, w_y, b_y, conv_w, conv_b, w_a, b_a, w_i, b_i, a_param, w_out, b_out, fwd_perm, back_perm, cp_size, tp_size):
    cp_index = lax.axis_index("cp")
    batch, n_tok, width = x_in.shape
    c_own = w_x.shape[1]
    n_own = c_own // CB
    swap_core = [(j, j ^ 1) for j in range(cp_size)]
    swap_x = [(j, j ^ 2) for j in range(cp_size)]

    slope = -8.0 * jax.nn.softplus(a_param)
    rows = [b_x, b_y, conv_b, b_a, b_i, slope, *[conv_w[k] for k in range(CONV_WIDTH)]]
    par = jnp.stack([r.astype(F32) for r in rows] + [jnp.zeros_like(slope)] * (PAR_ROWS - len(rows)))
    par = par.reshape(PAR_ROWS, n_own, CB).transpose(1, 0, 2)
    wg = jnp.concatenate([w_a, w_i], axis=-1).astype(F32).reshape(n_own, EXT_PAR, CB)
    ext = jnp.concatenate([wg, par, jnp.zeros((n_own, 6 * EXT_ROWS - EXT_PAR - PAR_ROWS, CB), F32)], axis=1)

    core = jnp.full((1,), cp_index % 2, jnp.int32)
    mine = send_pass(core, w_x, w_y, w_out, ext)
    to_y, to_z = [[(k, k ^ m) for k in range(tp_size)] for m in (1, 2)]
    got = {}
    for p in range(n_own):
        for u in range(2):
            got["y", p, u] = lax.ppermute(mine[2 * p + u], "tp", to_y)
            got["z", p, u] = lax.ppermute(mine[2 * p + u], "tp", to_z)
    for p in range(n_own):
        got["d", p, 0] = lax.ppermute(got["y", p, 0], "tp", to_z)
        got["d", p, 1] = lax.ppermute(got["z", p, 1], "tp", to_y)

    def blocks(keys):
        lst = []
        for way, p in keys:
            pair = [got[way, p, u] for u in range(2)]
            lst += pair
            for arr in pair:
                lst.append(lax.ppermute(arr, "cp", swap_core))
        return lst

    normed, gz_t, inv_b, gb_part = pre_pass(after(x_in, *mine), grad_z, norm_scale.astype(F32).reshape(1, width))
    n_halo = lax.ppermute(normed[n_tok - HALO:].astype(F32), "cp", fwd_perm).reshape(HALO * batch, width)
    normed = normed.reshape(n_tok * batch, width)
    gz_t = gz_t.reshape(n_tok * batch, width)
    pos_b = jnp.broadcast_to(seg_pos.T[:, :, None], (n_tok, batch, LANES))
    flat = lambda arr: arr.reshape(n_tok * batch, -1)

    c_o, y_o, g_o, q_o, info_o, xb_o, xh_o = first_pass(n_own, normed, gz_t, n_halo, pos_b, [w_x, w_y, w_out], ext)
    enter_o = entering(info_o, cp_index, swap_core, swap_x)
    mix_o, dpy_o, dbr_o, head_o, tail_o, acc, g_gate = second_pass(c_o, y_o, g_o, q_o, pos_b, enter_o, ext, xb_o, xh_o)
    back_o = lax.ppermute(head_o, "cp", back_perm)
    dbr_o = dbr_o.at[n_tok - HALO:].set((tail_o + back_o).astype(BF16))
    g_w_out = dot_tn(flat(mix_o), gz_t)
    g_w_y = dot_tn(normed, flat(dpy_o))
    g_w_x = dot_tn(after(normed, g_w_y, g_w_out), flat(dbr_o))

    calls = [[("y", 0), ("z", 0), ("y", 1)], [("z", 1), ("y", 2), ("z", 2)], [("d", 0), ("d", 1), ("d", 2)]]
    mixes, dpys, dbrs, w_far = [mix_o], [dpy_o], [dbr_o], []
    firsts = {}
    last = g_w_x
    for kind, idx in (("first", 0), ("second", 0), ("first", 1), ("first", 2), ("second", 1), ("second", 2)):
        if kind == "first":
            rows_n = after(normed, last)
            arrays = blocks(calls[idx])
            *acts, last, ext_f, w16 = first_pass(len(calls[idx]), rows_n, gz_t, n_halo, pos_b, arrays)
            firsts[idx] = acts, entering(last, cp_index, swap_core, swap_x), ext_f
            w_far.append(w16)
            continue
        (conv, *acts), enter_f, ext_f = firsts[idx]
        conv = after(conv, last)
        last, dpy_f, dbr_f, head_f, tail_f = second_pass(conv, *acts, pos_b, enter_f, ext_f)
        back_f = lax.ppermute(head_f, "cp", back_perm)
        dbr_f = dbr_f.at[n_tok - HALO:].set((tail_f + back_f).astype(BF16))
        for lst, val in zip((mixes, dpys, dbrs), (last, dpy_f, dbr_f)):
            lst.append(val)
    grad_x, gs_part = norm_back_pass(dbrs, dpys, w_x, w_y, w_far, x_in, inv_b, grad_z, norm_scale.astype(F32).reshape(1, width))
    acc = acc.reshape(c_own // LANES, N_ACC, 8, LANES).sum(axis=2).transpose(1, 0, 2).reshape(N_ACC, c_own)
    g_b_x = acc[:1] + jnp.sum(back_o, axis=(0, 1))
    g_a_param = -8.0 * jax.nn.sigmoid(a_param) * acc[4:5]
    g_b_out = jnp.sum(gb_part, axis=0).reshape(-1, c_own)
    smalls = jnp.concatenate([g_b_x, acc[1:4], g_a_param, acc[5:], g_b_out])
    n_small = smalls.shape[0]
    packed = jnp.concatenate([g_gate.reshape(-1, CB), jnp.pad(smalls, ((0, PAR_ROWS - n_small), (0, 0))).reshape(-1, CB)])
    g_w_x, g_w_y, g_w_out, packed = lax.psum((g_w_x, g_w_y, g_w_out, packed), "cp")
    g_gate = packed[:c_own].reshape(g_gate.shape)
    g_w_a, g_w_i = g_gate[:, :, :LANES], g_gate[:, :, LANES:]
    smalls = packed[c_own:].reshape(PAR_ROWS, c_own)
    g_b_x, g_b_y, g_b_a, g_b_i, g_a_param, g_conv_b = [smalls[k] for k in range(6)]
    g_conv_w, g_b_out = smalls[6:6 + CONV_WIDTH], smalls[6 + CONV_WIDTH:n_small].reshape(-1)
    g_scale = jnp.sum(gs_part, axis=0)
    g_scale = g_scale + sum(lax.ppermute(g_scale, "cp", [(j, j ^ m) for j in range(cp_size)]) for m in range(1, cp_size))
    mixes[0] = after(mixes[0], gs_part)
    z_out, g_w_x, g_w_y, g_w_out = out_pass(mixes, w_out, w_far, x_in, b_out.astype(F32).reshape(1, width), (g_w_x, g_w_y, g_w_out))
    return (z_out, grad_x, g_scale, g_w_x, g_b_x, g_w_y, g_b_y, g_conv_w, g_conv_b, g_w_a, g_b_a, g_w_i, g_b_i, g_a_param, g_w_out, g_b_out)


def solution(mesh):
    cp_size = mesh.shape["cp"]
    fwd_perm = [(j, j + 1) for j in range(cp_size - 1)]
    back_perm = [(j + 1, j) for j in range(cp_size - 1)]

    def per_device(*args):
        return shard_body(*args, fwd_perm=fwd_perm, back_perm=back_perm, cp_size=cp_size, tp_size=mesh.shape["tp"])

    return jax.shard_map(per_device, mesh=mesh, in_specs=IN_SPECS, out_specs=OUT_SPECS, check_vma=False)
```

```python
import functools
import jax
import jax.numpy as jnp
from jax import lax
from jax.experimental import pallas as pl
from jax.experimental.pallas import tpu as pltpu
from jax.sharding import PartitionSpec as P

NORM_EPS = 1e-6
CONV_WIDTH = 4
HALO = CONV_WIDTH - 1
LANES = 128
CB = 256
TC = 16
TINY = 1.2e-38
GELU_A = 0.7978845608028654
GELU_B = 0.044715
VMEM_BYTES = 67043328
F32 = jnp.float32
BF16 = jnp.bfloat16
TOKENS, COLS, CHANNEL = P(None, "cp"), P(None, "tp"), P("tp")
PARAM_SPECS = (P(), COLS, CHANNEL, COLS, CHANNEL, COLS, CHANNEL, CHANNEL, CHANNEL, CHANNEL, CHANNEL, CHANNEL, CHANNEL, P())
IN_SPECS = (TOKENS, TOKENS, TOKENS, *PARAM_SPECS)
OUT_SPECS = (TOKENS, TOKENS, *PARAM_SPECS)
R_BX, R_BY, R_CB, R_BA, R_BI, R_K, R_CW = range(7)
PAR_ROWS = 16
EXT_ROWS = 48
EXT_PAR = 256
N_TILE = 512
SUB = 8
B_BLK = 16


def dot_nn(lhs, rhs):
    return jnp.dot(lhs, rhs, preferred_element_type=F32)


def dot_nt(lhs, rhs):
    return lax.dot_general(lhs, rhs, (((1,), (1,)), ((), ())), preferred_element_type=F32)


def dot_tn(lhs, rhs):
    return lax.dot_general(lhs, rhs, (((0,), (0,)), ((), ())), preferred_element_type=F32)


def round16(val):
    return val.astype(BF16).astype(F32)


def sigmoid(val):
    return 1.0 / (1.0 + jnp.exp(-val))


def gates(pre_a, pre_i, slope, keep):
    gate_r = sigmoid(pre_a)
    gate_i = sigmoid(pre_i)
    log_a = gate_r * slope
    raw_a = jnp.exp(log_a)
    gap = jnp.tanh(-log_a) * (1.0 + raw_a * raw_a)
    inv_m = lax.rsqrt(jnp.maximum(gap, TINY))
    decay = jnp.where(keep, raw_a, 0.0)
    mult = jnp.where(keep, gap * inv_m, 1.0)
    return gate_r, gate_i, decay, mult, inv_m


def first_pass_kernel(n_ref, gz_ref, nh_ref, pos_ref, *rest, n_blk, n_chunk, own, batch):
    if own:
        ext, rest = rest[0], rest[1:]
        w_hbm, rest = rest[:3], rest[3:]
        c_out, y_out, g_out, q_out, info_out, xb_out, xh, w16, wo16, w_sem, xs, ys, ds, pre, tail, state = rest
    else:
        w_hbm, rest = rest[:4 * n_blk], rest[4 * n_blk:]
        c_out, y_out, g_out, q_out, info_out, ext, w_out, w16, stage, w_sem, o_sem, xs, ys, ds, pre, xh, tail, state = rest
        xb_out = None
    step = pl.program_id(0)
    width = n_ref.shape[1]
    quarter = width // 4

    def own_loads(blk):
        cols = pl.ds(blk * CB, CB)
        pair = [pltpu.make_async_copy(w_hbm[k].at[:, cols], w16.at[blk, k], w_sem.at[blk, k]) for k in range(2)]
        return pair + [pltpu.make_async_copy(w_hbm[2].at[cols, :], wo16.at[blk], w_sem.at[blk, 2])]

    def far_load(idx):
        return pltpu.make_async_copy(w_hbm[idx], stage.at[idx % 4], w_sem.at[idx])

    def stores(blk):
        return [pltpu.make_async_copy(w16.at[blk, k], w_out.at[k, :, pl.ds(blk * CB, CB)], o_sem.at[blk, k]) for k in range(3)]

    def dots(blk):
        rows = n_ref[:]
        xs[blk] = dot_nn(rows, w16[blk, 0])
        ys[blk] = dot_nn(rows, w16[blk, 1])
        ds[blk] = dot_nt(gz_ref[:], wo16[blk]) if own else dot_nn(gz_ref[:], w16[blk, 2])

    def fetch(blk):
        if own:
            for copy in own_loads(blk):
                copy.wait()
        else:
            core = lax.rem(lax.axis_index("cp"), 2)
            for i in range(4):
                far_load(4 * blk + i).wait()
                side = core if i < 2 else 1 - core
                start = pl.multiple_of((2 * side + i % 2) * quarter, quarter)
                for k in range(3):
                    w16[blk, k, pl.ds(start, quarter), :] = stage[i, k, :quarter].astype(BF16)
                    if i < 2:
                        ext[blk, (3 * i + k) * EXT_ROWS:(3 * i + k + 1) * EXT_ROWS] = stage[i, k, quarter:]
                if blk + 1 < n_blk:
                    far_load(4 * blk + 4 + i).start()
            for copy in stores(blk):
                copy.start()
        xh[blk] = dot_nn(nh_ref[:].astype(BF16), w16[blk, 0])

    def elementwise(blk):
        first = step == 1
        for half in range(CB // LANES):
            lane = slice(half * LANES, (half + 1) * LANES)
            row = lambda idx: ext[blk, EXT_PAR + idx:EXT_PAR + idx + 1, lane]
            bias_x, conv_b = row(R_BX), row(R_CB)
            taps = [row(R_CW + k) for k in range(CONV_WIDTH)]
            past = []
            for j in range(HALO):
                sl = slice(j * batch, (j + 1) * batch)
                past.append(jnp.where(first, round16(xh[blk, sl, lane] + bias_x), tail[blk, sl, lane]))
            for t in range(TC):
                sl = slice(t * batch, (t + 1) * batch)
                cur = round16(xs[blk, sl, lane] + bias_x)
                if own:
                    xb_out[blk, t, :, lane] = cur.astype(BF16)
                pos = pos_ref[t]
                total = conv_b + cur * taps[0]
                for k in range(1, CONV_WIDTH):
                    total = total + jnp.where(pos >= k, past[HALO - k], 0.0) * taps[k]
                c_out[blk, t, :, lane] = total.astype(BF16)
                past = past[1:] + [cur]
            for j in range(HALO):
                tail[blk, j * batch:(j + 1) * batch, lane] = past[j]
            wg = ext[blk, half * LANES:(half + 1) * LANES].astype(BF16)
            pre[half] = dot_nn(c_out[blk, :, :, lane].reshape(TC * batch, LANES), wg)
            bias_y, bias_a, bias_i, slope = row(R_BY), row(R_BA), row(R_BI), row(R_K)
            hid = jnp.where(first, 0.0, state[blk, 0, :, lane])
            prod = jnp.where(first, 1.0, state[blk, 1, :, lane])
            head = jnp.where(first, 0.0, state[blk, 2, :, lane])
            for t in range(TC):
                sl = slice(t * batch, (t + 1) * batch)
                keep = pos_ref[t] >= 1
                conv = c_out[blk, t, :, lane].astype(F32)
                _, gate_i, decay, mult, _ = gates(pre[half, sl, :LANES] + bias_a, pre[half, sl, LANES:] + bias_i, slope, keep)
                hid = decay * hid + mult * gate_i * conv
                prod = prod * decay
                pre_y = ys[blk, sl, lane] + bias_y
                sq = pre_y * pre_y
                tan = jnp.tanh(pre_y * (GELU_A + GELU_A * GELU_B * sq))
                half_y = 0.5 * pre_y
                d_mixed = ds[blk, sl, lane]
                y_act = half_y + half_y * tan
                slope_y = 0.5 + 0.5 * tan + half_y * (1.0 - tan * tan) * (GELU_A + 3.0 * GELU_A * GELU_B * sq)
                grad_h = d_mixed * y_act
                head = head + prod * grad_h
                y_out[blk, t, :, lane] = y_act
                g_out[blk, t, :, lane] = grad_h
                q_out[blk, t, :, lane] = d_mixed * slope_y
            for idx, val in enumerate((hid, prod, head)):
                state[blk, idx, :, lane] = val
                info_out[blk, idx, :, lane] = val

    @pl.when(step == 0)
    def _():
        if own:
            for blk in range(n_blk):
                for copy in own_loads(blk):
                    copy.start()
        else:
            for i in range(4):
                far_load(i).start()
        for blk in range(n_blk):
            fetch(blk)
            dots(blk)

    @pl.when((step > 0) & (step < n_chunk))
    def _():
        def both(blk, _):
            elementwise(blk)
            dots(blk)
            return 0

        if own:
            for blk in range(n_blk):
                both(blk, 0)
        else:
            lax.fori_loop(0, n_blk, both, 0)

    @pl.when(step == n_chunk)
    def _():
        def last(blk, _):
            elementwise(blk)
            return 0

        lax.fori_loop(0, n_blk, last, 0)
        if not own:
            for blk in range(n_blk):
                for copy in stores(blk):
                    copy.wait()


def first_pass(n_blk, normed, gz, n_halo, pos_b, weights, ext=None):
    own = ext is not None
    n_rows, width = normed.shape
    n_tok, batch = pos_b.shape[0], pos_b.shape[1]
    n_chunk = n_tok // TC
    cols = n_blk * CB
    rows = TC * batch
    cur = lambda s: jnp.minimum(s, n_chunk - 1)
    old = lambda s: jnp.maximum(s - 1, 0)
    const = lambda shape: pl.BlockSpec(shape, lambda s: (0,) * len(shape))
    row_spec = pl.BlockSpec((rows, width), lambda s: (cur(s), 0))
    any_spec = pl.BlockSpec(memory_space=pl.ANY)
    in_specs = [row_spec, row_spec, const((HALO * batch, width)), pl.BlockSpec((TC, batch, LANES), lambda s: (old(s), 0, 0))]
    tok_spec = pl.BlockSpec((n_blk, TC, batch, CB), lambda s: (0, old(s), 0, 0))
    tok_shape = lambda dt: jax.ShapeDtypeStruct((n_blk, n_tok, batch, CB), dt)
    ext_shape = (n_blk, 6 * EXT_ROWS, CB)
    out_specs = [tok_spec] * 4 + [const((n_blk, 3, batch, CB))]
    out_shape = [tok_shape(BF16), tok_shape(F32), tok_shape(F32), tok_shape(F32), jax.ShapeDtypeStruct((n_blk, 3, batch, CB), F32)]
    work = [pltpu.VMEM((n_blk, rows, CB), F32)] * 3 + [pltpu.VMEM((CB // LANES, rows, 2 * LANES), F32)]
    halo = pltpu.VMEM((n_blk, HALO * batch, CB), F32)
    state = pltpu.VMEM((n_blk, 3, batch, CB), F32)
    args = [normed, gz, n_halo, pos_b]
    if own:
        in_specs.append(const(ext_shape))
        args.append(ext)
        out_specs += [tok_spec, const((n_blk, HALO * batch, CB))]
        out_shape += [tok_shape(BF16), jax.ShapeDtypeStruct((n_blk, HALO * batch, CB), F32)]
        scratch = [pltpu.VMEM((n_blk, 2, width, CB), BF16), pltpu.VMEM((n_blk, CB, width), BF16), pltpu.SemaphoreType.DMA((n_blk, 3)), *work, halo, state]
    else:
        out_specs += [const(ext_shape), any_spec]
        out_shape += [jax.ShapeDtypeStruct(ext_shape, F32), jax.ShapeDtypeStruct((3, width, cols), BF16)]
        scratch = [pltpu.VMEM((n_blk, 3, width, CB), BF16), pltpu.VMEM((4, *weights[0].shape), F32), pltpu.SemaphoreType.DMA((4 * n_blk,)), pltpu.SemaphoreType.DMA((n_blk, 3)), *work, halo, halo, state]
    in_specs += [any_spec] * len(weights)
    flops = 6 * n_rows * width * cols
    return pl.pallas_call(
        functools.partial(first_pass_kernel, n_blk=n_blk, n_chunk=n_chunk, own=own, batch=batch),
        grid=(n_chunk + 1,), in_specs=in_specs, out_specs=out_specs, scratch_shapes=scratch, out_shape=out_shape,
        compiler_params=pltpu.CompilerParams(dimension_semantics=("arbitrary",), vmem_limit_bytes=VMEM_BYTES),
        cost_estimate=pl.CostEstimate(flops=flops, bytes_accessed=n_rows * width * 4, transcendentals=0),
        name="first_pass_own" if own else "first_pass_far",
    )(*args, *weights)


def turned(val):
    return jnp.swapaxes(val, 0, 1)


def lane_tiles(width):
    return [slice(k, k + LANES) for k in range(0, width, LANES)]


def pre_kernel(x_ref, gz_ref, s_ref, n_out, gz_out, inv_out, gb_out):
    width = x_ref.shape[2]
    total = 0.0
    for lane in lane_tiles(width):
        x_f = x_ref[:, :, lane].astype(F32)
        total = total + x_f * x_f
    inv_out[:] = jnp.broadcast_to(lax.rsqrt(jnp.sum(total, axis=-1, keepdims=True) * (1.0 / width) + NORM_EPS), inv_out.shape)

    @pl.when(pl.program_id(0) == 0)
    def _():
        gb_out[:] = jnp.zeros_like(gb_out)

    for lane in lane_tiles(width):
        normed = x_ref[:, :, lane].astype(F32) * inv_out[:] * (1.0 + s_ref[:, lane])
        n_out[:, :, lane] = turned(normed).astype(BF16)
        gz_f = gz_ref[:, :, lane].astype(F32)
        gz_out[:, :, lane] = turned(gz_f).astype(BF16)
        gb_out[:, lane] += jnp.sum(gz_f.reshape(-1, SUB, LANES), axis=0)


def row_specs(batch, n_tok, b_blk=B_BLK):
    per = batch // b_blk
    n_steps = (n_tok // TC) * per
    cur = lambda s: jnp.minimum(s, n_steps - 1)
    old = lambda s: jnp.maximum(s - 1, 0)
    act = lambda lanes: pl.BlockSpec((TC, b_blk, lanes), lambda s: (cur(s) // per, lax.rem(cur(s), per), 0))
    native = lambda lag, lanes: pl.BlockSpec((b_blk, TC, lanes), lambda s: (lax.rem(lag(s), per), lag(s) // per, 0))
    return n_steps, cur, old, act, native


def pre_pass(x_in, grad_z, scale):
    batch, n_tok, width = x_in.shape
    n_steps, cur, _, act, native = row_specs(batch, n_tok, batch)
    const = lambda shape: pl.BlockSpec(shape, lambda s: (0,) * len(shape))
    return pl.pallas_call(
        pre_kernel, grid=(n_steps,),
        in_specs=[native(cur, width), native(cur, width), const((1, width))], out_specs=[act(width), act(width), native(cur, LANES), const((SUB, width))],
        out_shape=[jax.ShapeDtypeStruct((n_tok, batch, width), BF16)] * 2 + [jax.ShapeDtypeStruct((batch, n_tok, LANES), F32), jax.ShapeDtypeStruct((SUB, width), F32)],
        compiler_params=pltpu.CompilerParams(dimension_semantics=("arbitrary",), vmem_limit_bytes=VMEM_BYTES),
        cost_estimate=pl.CostEstimate(flops=n_tok * batch * width * 200, bytes_accessed=n_tok * batch * width * 8, transcendentals=0),
        name="pre_pass",
    )(x_in, grad_z, scale)


def send_kernel(core_ref, wx_ref, wy_ref, wo_ref, ext_ref, *outs):
    quarter = wx_ref.shape[0]
    for idx, out in enumerate(outs):
        @pl.when(pl.program_id(0) == idx)
        def _():
            values = wx_ref[:].astype(F32), wy_ref[:].astype(F32), wo_ref[:].astype(F32).T
            for k, val in enumerate(values):
                out[k, :quarter] = val
                out[k, quarter:] = ext_ref[0, k * EXT_ROWS:(k + 1) * EXT_ROWS]


def send_pass(core, w_x, w_y, w_out, ext):
    (width, _), n_own = w_x.shape, len(ext)
    quarter = width // 4
    tall = pl.BlockSpec((quarter, CB), lambda i, core: (2 * core[0] + lax.rem(i, 2), i // 2))
    wide = pl.BlockSpec((CB, quarter), lambda i, core: (i // 2, 2 * core[0] + lax.rem(i, 2)))
    shape = (3, quarter + EXT_ROWS, CB)
    return pl.pallas_call(
        send_kernel,
        grid_spec=pltpu.PrefetchScalarGridSpec(num_scalar_prefetch=1, grid=(2 * n_own,), in_specs=[tall, tall, wide, pl.BlockSpec((1, 3 * EXT_ROWS, CB), lambda i, core: (i // 2, lax.rem(i, 2), 0))],
                                               out_specs=[pl.BlockSpec(shape, lambda i, core: (0, 0, 0))] * (2 * n_own)),
        out_shape=[jax.ShapeDtypeStruct(shape, F32)] * (2 * n_own),
        compiler_params=pltpu.CompilerParams(dimension_semantics=("arbitrary",), vmem_limit_bytes=VMEM_BYTES),
        cost_estimate=pl.CostEstimate(flops=10 ** 9, bytes_accessed=2 * 10 ** 7, transcendentals=0),
        name="send_pass",
    )(core, w_x, w_y, w_out, ext)


N_ACC = 10
ACC_ROWS = 8 * N_ACC


def second_pass_kernel(c_ref, y_ref, g_ref, q_ref, pos_ref, enter_ref, wg_ref, par_ref, *rest, n_chunk, own, batch):
    if own:
        xb_ref, xh_ref, mix_out, dpy_out, dbr_out, head_out, tail_out, acc_out, gw_out, s_a, s_A, s_i, s_m, pre, dpai, dgate, s_e = rest
    else:
        mix_out, dpy_out, dbr_out, head_out, tail_out, s_a, s_A, s_i, s_m, pre, dpai, dgate = rest
    row = lambda idx: par_ref[0, idx:idx + 1, :]
    wg = wg_ref[0].astype(BF16)
    enter = (enter_ref[0, 0], enter_ref[0, 1])
    bias_a, bias_i, slope = row(R_BA), row(R_BI), row(R_K)
    taps = [row(R_CW + k) for k in range(CONV_WIDTH)]

    def add(idx, val):
        acc_out[0, pl.ds(8 * idx, 8)] = acc_out[0, pl.ds(8 * idx, 8)] + val

    fold = lambda val: jnp.sum(val.reshape(batch // 8, 8, LANES), axis=0)
    if own:
        halo = [round16(xh_ref[0, k * batch:(k + 1) * batch] + row(R_BX)) for k in range(HALO)]
        acc_out[:] = jnp.zeros_like(acc_out)
        gw_out[:] = jnp.zeros_like(gw_out)

    def chunk_of(j):
        return c_ref[0, pl.ds(j * TC, TC)].reshape(TC * batch, LANES)

    def pre_gates(j):
        pre[:] = dot_nn(chunk_of(j), wg)

    def forward(j, hid):
        base = j * TC
        acc_y = jnp.zeros((8, LANES), F32)
        for t in range(TC):
            sl = slice(t * batch, (t + 1) * batch)
            tok = base + t
            keep = pos_ref[tok] >= 1
            conv = c_ref[0, tok].astype(F32)
            gate_r, gate_i, decay, mult, inv_m = gates(pre[sl, :LANES] + bias_a, pre[sl, LANES:] + bias_i, slope, keep)
            in_conv = gate_i * conv
            before = hid
            hid = decay * before + mult * in_conv
            d_log = decay * (before - in_conv * decay * inv_m)
            r_log = d_log * gate_r
            s_a[tok] = decay
            s_A[tok] = r_log * (1.0 - gate_r) * slope
            s_i[tok] = mult * in_conv * (1.0 - gate_i)
            s_m[tok] = mult * gate_i
            mix_out[tok] = (hid * y_ref[0, tok]).astype(BF16)
            d_pre_y = hid * q_ref[0, tok]
            dpy_out[tok] = d_pre_y.astype(BF16)
            if own:
                s_e[tok] = r_log
                acc_y = acc_y + fold(d_pre_y)
        if own:
            add(1, acc_y)
        pre_gates(jnp.minimum(j + 1, n_chunk - 1))
        return hid

    pre_gates(0)
    lax.fori_loop(0, n_chunk, forward, enter[0])

    def recur(j, carry):
        base = j * TC
        acc_a = acc_i = acc_p = jnp.zeros((8, LANES), F32)
        for t in range(TC - 1, -1, -1):
            sl = slice(t * batch, (t + 1) * batch)
            tok = base + t
            grad_h = g_ref[0, tok] + carry
            carry = s_a[tok] * grad_h
            d_pre_a = grad_h * s_A[tok]
            d_pre_i = grad_h * s_i[tok]
            s_m[tok] = grad_h * s_m[tok]
            dpai[sl, :LANES] = d_pre_a.astype(BF16)
            dpai[sl, LANES:] = d_pre_i.astype(BF16)
            if own:
                acc_a = acc_a + fold(d_pre_a)
                acc_i = acc_i + fold(d_pre_i)
                acc_p = acc_p + fold(grad_h * s_e[tok])
        if own:
            add(2, acc_a)
            add(3, acc_i)
            add(4, acc_p)
            gw_out[0] = gw_out[0] + dot_tn(chunk_of(j), dpai[:])
        return carry

    def conv_back(j, later):
        base = j * TC
        later = list(later)
        acc_x = acc_b = jnp.zeros((8, LANES), F32)
        acc_w = [jnp.zeros((8, LANES), F32) for _ in range(CONV_WIDTH)]
        for t in range(TC - 1, -1, -1):
            sl = slice(t * batch, (t + 1) * batch)
            tok = base + t
            d_conv = s_m[tok] + dgate[sl]
            total = d_conv * taps[0] + later[0]
            pos = pos_ref[tok]
            masked = [jnp.where(pos >= k, d_conv, 0.0) for k in range(1, CONV_WIDTH)]
            later = [later[1] + masked[0] * taps[1], later[2] + masked[1] * taps[2], masked[2] * taps[3]]
            dbr_out[tok] = total.astype(BF16)
            if t >= TC - HALO:
                tail_out[t - (TC - HALO)] = jnp.where(j == n_chunk - 1, total, tail_out[t - (TC - HALO)])
            if own:
                acc_x = acc_x + fold(total)
                acc_b = acc_b + fold(d_conv)
                acc_w[0] = acc_w[0] + fold(d_conv * xb_ref[0, tok].astype(F32))
                for k in range(1, CONV_WIDTH):
                    past = xb_ref[0, jnp.maximum(tok - k, 0)].astype(F32)
                    if t < k:
                        past = jnp.where(j == 0, halo[HALO + t - k], past)
                    acc_w[k] = acc_w[k] + fold(masked[k - 1] * past)
        if own:
            add(0, acc_x)
            add(5, acc_b)
            for k in range(CONV_WIDTH):
                add(6 + k, acc_w[k])
        return tuple(later)

    tail_out[:] = jnp.zeros_like(tail_out)
    zero = jnp.zeros((batch, LANES), F32)
    carry = recur(n_chunk - 1, enter[1])
    dgate[:] = dot_nt(dpai[:], wg)

    def back(idx, vals):
        carry, later = vals[0], vals[1:]
        j = n_chunk - 2 - idx
        carry = recur(j, carry)
        later = conv_back(j + 1, later)
        dgate[:] = dot_nt(dpai[:], wg)
        return (carry, *later)

    vals = lax.fori_loop(0, n_chunk - 1, back, (carry, zero, zero, zero))
    later = conv_back(0, vals[1:])
    for k in range(HALO):
        head_out[HALO - 1 - k] = later[k]


def second_pass(conv, y_act, grad_h, q_val, pos_b, enter, ext, xb=None, xb_halo=None):
    own = xb is not None
    n_blk, n_tok, batch, _ = conv.shape
    n_chunk = n_tok // TC
    per = CB // LANES
    cols = n_blk * CB
    tok_spec = pl.BlockSpec((1, n_tok, batch, LANES), lambda s: (s // per, 0, 0, lax.rem(s, per)))
    lane_spec = lambda n: pl.BlockSpec((n, batch, LANES), lambda s: (0, 0, s))
    in_specs = [tok_spec] * 4 + [pl.BlockSpec((n_tok, batch, LANES), lambda s: (0, 0, 0)),
                pl.BlockSpec((1, 2, batch, LANES), lambda s: (s // per, 0, 0, lax.rem(s, per))),
                pl.BlockSpec((1, LANES, CB), lambda s: (s // per, lax.rem(s, per), 0)),
                pl.BlockSpec((1, PAR_ROWS, LANES), lambda s: (s // per, EXT_PAR // PAR_ROWS, lax.rem(s, per)))]
    out_specs = [lane_spec(n_tok)] * 3 + [lane_spec(HALO)] * 2
    out_shape = [jax.ShapeDtypeStruct((n_tok, batch, cols), BF16)] * 3 + [jax.ShapeDtypeStruct((HALO, batch, cols), F32)] * 2
    scratch = [pltpu.VMEM((n_tok, batch, LANES), F32)] * 4 + [pltpu.VMEM((TC * batch, 2 * LANES), F32), pltpu.VMEM((TC * batch, 2 * LANES), BF16), pltpu.VMEM((TC * batch, LANES), F32)]
    args = [conv, y_act, grad_h, q_val, pos_b, enter, ext, ext]
    if own:
        in_specs += [tok_spec, pl.BlockSpec((1, HALO * batch, LANES), lambda s: (s // per, 0, lax.rem(s, per)))]
        out_specs += [pl.BlockSpec((1, ACC_ROWS, LANES), lambda s: (s, 0, 0)), pl.BlockSpec((1, LANES, 2 * LANES), lambda s: (s, 0, 0))]
        out_shape += [jax.ShapeDtypeStruct((n_blk * per, ACC_ROWS, LANES), F32), jax.ShapeDtypeStruct((n_blk * per, LANES, 2 * LANES), F32)]
        scratch.append(pltpu.VMEM((n_tok, batch, LANES), F32))
        args += [xb, xb_halo]
    n_elem = n_tok * batch * cols
    return pl.pallas_call(
        functools.partial(second_pass_kernel, n_chunk=n_chunk, own=own, batch=batch),
        grid=(n_blk * per,), in_specs=in_specs, out_specs=out_specs, scratch_shapes=scratch, out_shape=out_shape,
        compiler_params=pltpu.CompilerParams(dimension_semantics=("arbitrary",), vmem_limit_bytes=VMEM_BYTES),
        cost_estimate=pl.CostEstimate(flops=n_elem * 12000, bytes_accessed=n_elem * 20, transcendentals=n_elem * 6),
        name="second_pass_own" if own else "second_pass_far",
    )(*args)


def tile_of(j):
    return pl.ds(pl.multiple_of(j * N_TILE, N_TILE), N_TILE)


def out_kernel(*refs, n_part, n_steps, n_pass):
    mixes, refs = refs[:n_part], refs[n_part:]
    w_hbm, refs = refs[:n_part], refs[n_part:]
    pass_in, refs = refs[:n_pass], refs[n_pass:]
    x_ref, b_ref, z_ref, refs = refs[0], refs[1], refs[2], refs[3:]
    pass_out, refs = refs[:n_pass], refs[n_pass:]
    w_v, acc, sem = refs[:n_part], refs[n_part], refs[n_part + 1]
    rows = TC * B_BLK
    n_tiles = z_ref.shape[2] // N_TILE
    step = pl.program_id(0)

    def copies(j):
        tile = tile_of(j)
        first = pltpu.make_async_copy(w_hbm[0].at[:, tile], w_v[0].at[:, tile], sem.at[j, 0])
        return [first] + [pltpu.make_async_copy(w_hbm[i].at[2, tile, :], w_v[i].at[tile, :], sem.at[j, i]) for i in range(1, n_part)]

    def product(tile):
        proj = dot_nn(mixes[0][:].reshape(rows, -1), w_v[0][:, tile])
        for i in range(1, n_part):
            proj = proj + dot_nt(mixes[i][:].reshape(rows, -1), w_v[i][tile, :])
        acc[:, tile] = proj

    def finish():
        for lane in lane_tiles(z_ref.shape[2]):
            proj = turned(acc[:, lane].reshape(TC, B_BLK, LANES))
            z_ref[:, :, lane] = (x_ref[:, :, lane].astype(F32) + (proj + b_ref[:, lane])).astype(BF16)
        for src, dst in zip(pass_in, pass_out):
            dst[:] = src[:]

    @pl.when(step == 0)
    def _():
        for j in range(n_tiles):
            for copy in copies(j):
                copy.start()

        def first(j, _):
            for copy in copies(j):
                copy.wait()
            product(tile_of(j))
            return 0

        lax.fori_loop(0, n_tiles, first, 0)

    @pl.when((step > 0) & (step < n_steps))
    def _():
        finish()
        product(slice(None))

    @pl.when(step == n_steps)
    def _():
        finish()


def out_pass(mixes, w_own, w_far, x_in, b_out, sums):
    n_tok, batch, _ = mixes[0].shape
    width = x_in.shape[2]
    n_steps, _, old, act, native = row_specs(batch, n_tok)
    n_part = len(mixes)
    any_spec = pl.BlockSpec(memory_space=pl.ANY)
    strips = [pl.BlockSpec((g.shape[0] // n_steps, g.shape[1]), lambda s: (old(s), 0)) for g in sums]
    return pl.pallas_call(
        functools.partial(out_kernel, n_part=n_part, n_steps=n_steps, n_pass=len(sums)), grid=(n_steps + 1,),
        in_specs=[act(m.shape[2]) for m in mixes] + [any_spec] * n_part + strips + [native(old, width), pl.BlockSpec((1, width), lambda s: (0, 0))],
        out_specs=[native(old, width)] + strips, out_shape=[jax.ShapeDtypeStruct(a.shape, a.dtype) for a in (x_in, *sums)],
        scratch_shapes=[pltpu.VMEM(w_own.shape, BF16)] + [pltpu.VMEM(w.shape[1:], BF16) for w in w_far] + [pltpu.VMEM((TC * B_BLK, width), F32), pltpu.SemaphoreType.DMA((width // N_TILE, n_part))],
        compiler_params=pltpu.CompilerParams(dimension_semantics=("arbitrary",), vmem_limit_bytes=VMEM_BYTES),
        cost_estimate=pl.CostEstimate(flops=2 * n_tok * batch * width * width, bytes_accessed=n_tok * batch * width * 8, transcendentals=0),
        name="out_pass",
    )(*mixes, w_own, *w_far, *sums, x_in, b_out)


def norm_back_kernel(*refs, n_part, n_steps):
    n_all = 2 * n_part
    lhs, refs = refs[:n_all], refs[n_all:]
    w_hbm, refs = refs[:n_part + 1], refs[n_part + 1:]
    x_ref, inv_ref, gz_ref, s_ref, gx_ref, gs_ref, *refs = refs
    w_v, (acc, d_n, x_old, sums, scale, shift, sem) = refs[:n_all], refs[n_all:]
    rows = TC * B_BLK
    width = gx_ref.shape[2]
    n_tiles = width // N_TILE
    wide = width // 2
    step = pl.program_id(0)

    def copies(j):
        tile = tile_of(j)
        lst = []
        for k in range(2):
            for i in range(n_part):
                src = w_hbm[k].at[tile, :] if i == 0 else w_hbm[i + 1].at[k, tile, :]
                idx = k * n_part + i
                lst.append(pltpu.make_async_copy(src, w_v[idx].at[tile, :], sem.at[j, idx]))
        return lst

    def product(tile):
        val = dot_nt(lhs[0][:].reshape(rows, -1), w_v[0][tile, :])
        for arr, weight in zip(lhs[1:], w_v[1:]):
            val = val + dot_nt(arr[:].reshape(rows, -1), weight[tile, :])
        acc[:, tile] = val

    def turn(tiles):
        for lane in tiles:
            val = turned(acc[:, lane].reshape(TC, B_BLK, LANES))
            d_n[:, :, lane] = val
            x_t = x_ref[:, :, lane]
            x_old[:, :, lane] = x_t
            sums[:] += val * (1.0 + s_ref[:, lane]) * x_t.astype(F32)

    def close():
        inv = inv_ref[:]
        scale[:] = inv
        shift[:] = inv * inv * inv * (jnp.sum(sums[:], axis=-1, keepdims=True) * (1.0 / width))
        sums[:] = jnp.zeros_like(sums)

    def finish():
        for lane in lane_tiles(width):
            val, inv = d_n[:, :, lane], scale[:]
            x_f = x_old[:, :, lane].astype(F32)
            gx_ref[:, :, lane] = (gz_ref[:, :, lane].astype(F32) + (inv * (val * (1.0 + s_ref[:, lane])) - x_f * shift[:])).astype(BF16)
            gs_ref[:, lane] += jnp.sum((val * x_f * inv).reshape(-1, SUB, LANES), axis=0)

    low, high = lane_tiles(width)[:wide // LANES], lane_tiles(width)[wide // LANES:]

    @pl.when(step == 0)
    def _():
        gs_ref[:] = jnp.zeros_like(gs_ref)
        sums[:] = jnp.zeros_like(sums)
        for j in range(n_tiles):
            for copy in copies(j):
                copy.start()

        def first(j, _):
            for copy in copies(j):
                copy.wait()
            product(tile_of(j))
            return 0

        lax.fori_loop(0, n_tiles, first, 0)
        turn(low + high)
        close()

    @pl.when((step > 0) & (step < n_steps))
    def _():
        finish()
        product(slice(wide))
        turn(low)
        product(slice(wide, None))
        turn(high)
        close()

    @pl.when(step == n_steps)
    def _():
        finish()


def norm_back_pass(dbrs, dpys, wx_own, wy_own, w_far, x_in, inv_b, grad_z, scale):
    n_tok, batch, _ = dbrs[0].shape
    width = x_in.shape[2]
    n_steps, cur, old, act, native = row_specs(batch, n_tok)
    n_part = len(dbrs)
    const = lambda shape: pl.BlockSpec(shape, lambda s: (0,) * len(shape))
    planes = [pltpu.VMEM(wx_own.shape, BF16)] + [pltpu.VMEM(w.shape[1:], BF16) for w in w_far]
    block = lambda dt, lanes: pltpu.VMEM((B_BLK, TC, lanes), dt)
    return pl.pallas_call(
        functools.partial(norm_back_kernel, n_part=n_part, n_steps=n_steps), grid=(n_steps + 1,),
        in_specs=[act(m.shape[2]) for m in (*dbrs, *dpys)] + [pl.BlockSpec(memory_space=pl.ANY)] * (n_part + 1) + [native(cur, width), native(cur, LANES), native(old, width), const((1, width))],
        out_specs=[native(old, width), const((SUB, width))],
        out_shape=[jax.ShapeDtypeStruct(x_in.shape, BF16), jax.ShapeDtypeStruct((SUB, width), F32)],
        scratch_shapes=[*planes, *planes, pltpu.VMEM((TC * B_BLK, width), F32), block(F32, width), block(BF16, width), *[block(F32, LANES)] * 3, pltpu.SemaphoreType.DMA((width // N_TILE, 2 * n_part))],
        compiler_params=pltpu.CompilerParams(dimension_semantics=("arbitrary",), vmem_limit_bytes=VMEM_BYTES),
        cost_estimate=pl.CostEstimate(flops=4 * n_tok * batch * width * width, bytes_accessed=n_tok * batch * width * 10, transcendentals=0),
        name="norm_back_pass",
    )(*dbrs, *dpys, wx_own, wy_own, *w_far, x_in, inv_b, grad_z, scale)


def after(val, *deps):
    return lax.optimization_barrier((val, *deps))[0]


def entering(info, cp_index, swap_core, swap_x):
    end, prod, head = [info[:, k] for k in range(3)]
    other = lax.ppermute(info, "cp", swap_core)
    o_end, o_prod, o_head = [other[:, k] for k in range(3)]
    upper_core = cp_index % 2 == 1
    upper_chip = cp_index >= 2
    chip_end = jnp.where(upper_core, prod * o_end + end, o_prod * end + o_end)
    chip_head = jnp.where(upper_core, o_head + o_prod * head, head + prod * o_head)
    got = lax.ppermute(jnp.where(upper_chip, chip_head, chip_end), "cp", swap_x)
    from_low = jnp.where(upper_chip, got, 0.0)
    from_high = jnp.where(upper_chip, 0.0, got)
    state_in = jnp.where(upper_core, o_prod * from_low + o_end, from_low)
    grad_in = jnp.where(upper_core, from_high, o_head + o_prod * from_high)
    return jnp.stack([state_in, grad_in], axis=1)


def shard_body(x_in, grad_z, seg_pos, norm_scale, w_x, b_x, w_y, b_y, conv_w, conv_b, w_a, b_a, w_i, b_i, a_param, w_out, b_out, fwd_perm, back_perm, cp_size, tp_size):
    cp_index = lax.axis_index("cp")
    batch, n_tok, width = x_in.shape
    c_own = w_x.shape[1]
    n_own = c_own // CB
    swap_core = [(j, j ^ 1) for j in range(cp_size)]
    swap_x = [(j, j ^ 2) for j in range(cp_size)]

    slope = -8.0 * jax.nn.softplus(a_param)
    rows = [b_x, b_y, conv_b, b_a, b_i, slope, *[conv_w[k] for k in range(CONV_WIDTH)]]
    par = jnp.stack([r.astype(F32) for r in rows] + [jnp.zeros_like(slope)] * (PAR_ROWS - len(rows)))
    par = par.reshape(PAR_ROWS, n_own, CB).transpose(1, 0, 2)
    wg = jnp.concatenate([w_a, w_i], axis=-1).astype(F32).reshape(n_own, EXT_PAR, CB)
    ext = jnp.concatenate([wg, par, jnp.zeros((n_own, 6 * EXT_ROWS - EXT_PAR - PAR_ROWS, CB), F32)], axis=1)

    x_halo = lax.ppermute(x_in[:, n_tok - HALO:].astype(F32).transpose(1, 0, 2), "cp", fwd_perm)
    core = jnp.full((1,), cp_index % 2, jnp.int32)
    mine = send_pass(core, w_x, w_y, w_out, ext)
    to_y, to_z = [[(k, k ^ m) for k in range(tp_size)] for m in (1, 2)]
    got = {}
    for p in range(n_own):
        for u in range(2):
            got["y", p, u] = lax.ppermute(mine[2 * p + u], "tp", to_y)
            got["z", p, u] = lax.ppermute(mine[2 * p + u], "tp", to_z)
    for p in range(n_own):
        got["d", p, 0] = lax.ppermute(got["y", p, 0], "tp", to_z)
        got["d", p, 1] = lax.ppermute(got["z", p, 1], "tp", to_y)

    def blocks(keys):
        lst = []
        for way, p in keys:
            pair = [got[way, p, u] for u in range(2)]
            lst += pair
            for arr in pair:
                lst.append(lax.ppermute(arr, "cp", swap_core))
        return lst

    normed, gz_t, inv_b, gb_part = pre_pass(after(x_in, *mine), grad_z, norm_scale.astype(F32).reshape(1, width))
    inv_h = lax.rsqrt(jnp.mean(x_halo * x_halo, axis=-1, keepdims=True) + NORM_EPS)
    n_halo = (x_halo * inv_h * (1.0 + norm_scale.astype(F32))).reshape(HALO * batch, width)
    normed = normed.reshape(n_tok * batch, width)
    gz_t = gz_t.reshape(n_tok * batch, width)
    pos_b = jnp.broadcast_to(seg_pos.T[:, :, None], (n_tok, batch, LANES))
    flat = lambda arr: arr.reshape(n_tok * batch, -1)

    c_o, y_o, g_o, q_o, info_o, xb_o, xh_o = first_pass(n_own, normed, gz_t, n_halo, pos_b, [w_x, w_y, w_out], ext)
    enter_o = entering(info_o, cp_index, swap_core, swap_x)
    mix_o, dpy_o, dbr_o, head_o, tail_o, acc, g_gate = second_pass(c_o, y_o, g_o, q_o, pos_b, enter_o, ext, xb_o, xh_o)
    back_o = lax.ppermute(head_o, "cp", back_perm)
    dbr_o = dbr_o.at[n_tok - HALO:].set((tail_o + back_o).astype(BF16))
    g_w_out = dot_tn(flat(mix_o), gz_t)
    g_w_y = dot_tn(normed, flat(dpy_o))
    g_w_x = dot_tn(after(normed, g_w_y, g_w_out), flat(dbr_o))

    calls = [[("y", 0), ("z", 0), ("y", 1)], [("z", 1), ("y", 2), ("z", 2)], [("d", 0), ("d", 1), ("d", 2)]]
    mixes, dpys, dbrs, w_far = [mix_o], [dpy_o], [dbr_o], []
    firsts = {}
    last = g_w_x
    for kind, idx in (("first", 0), ("second", 0), ("first", 1), ("first", 2), ("second", 1), ("second", 2)):
        if kind == "first":
            rows_n = after(normed, last)
            arrays = blocks(calls[idx])
            *acts, last, ext_f, w16 = first_pass(len(calls[idx]), rows_n, gz_t, n_halo, pos_b, arrays)
            firsts[idx] = acts, entering(last, cp_index, swap_core, swap_x), ext_f
            w_far.append(w16)
            continue
        (conv, *acts), enter_f, ext_f = firsts[idx]
        conv = after(conv, last)
        last, dpy_f, dbr_f, head_f, tail_f = second_pass(conv, *acts, pos_b, enter_f, ext_f)
        back_f = lax.ppermute(head_f, "cp", back_perm)
        dbr_f = dbr_f.at[n_tok - HALO:].set((tail_f + back_f).astype(BF16))
        for lst, val in zip((mixes, dpys, dbrs), (last, dpy_f, dbr_f)):
            lst.append(val)
    grad_x, gs_part = norm_back_pass(dbrs, dpys, w_x, w_y, w_far, x_in, inv_b, grad_z, norm_scale.astype(F32).reshape(1, width))
    acc = acc.reshape(c_own // LANES, N_ACC, 8, LANES).sum(axis=2).transpose(1, 0, 2).reshape(N_ACC, c_own)
    g_b_x = acc[:1] + jnp.sum(back_o, axis=(0, 1))
    g_a_param = -8.0 * jax.nn.sigmoid(a_param) * acc[4:5]
    g_b_out = jnp.sum(gb_part, axis=0).reshape(-1, c_own)
    smalls = jnp.concatenate([g_b_x, acc[1:4], g_a_param, acc[5:], g_b_out])
    n_small = smalls.shape[0]
    packed = jnp.concatenate([g_gate.reshape(-1, CB), jnp.pad(smalls, ((0, PAR_ROWS - n_small), (0, 0))).reshape(-1, CB)])
    g_w_x, g_w_y, g_w_out, packed = lax.psum((g_w_x, g_w_y, g_w_out, packed), "cp")
    g_gate = packed[:c_own].reshape(g_gate.shape)
    g_w_a, g_w_i = g_gate[:, :, :LANES], g_gate[:, :, LANES:]
    smalls = packed[c_own:].reshape(PAR_ROWS, c_own)
    g_b_x, g_b_y, g_b_a, g_b_i, g_a_param, g_conv_b = [smalls[k] for k in range(6)]
    g_conv_w, g_b_out = smalls[6:6 + CONV_WIDTH], smalls[6 + CONV_WIDTH:n_small].reshape(-1)
    g_scale = jnp.sum(gs_part, axis=0)
    g_scale = g_scale + sum(lax.ppermute(g_scale, "cp", [(j, j ^ m) for j in range(cp_size)]) for m in range(1, cp_size))
    mixes[0] = after(mixes[0], gs_part)
    z_out, g_w_x, g_w_y, g_w_out = out_pass(mixes, w_out, w_far, x_in, b_out.astype(F32).reshape(1, width), (g_w_x, g_w_y, g_w_out))
    return (z_out, grad_x, g_scale, g_w_x, g_b_x, g_w_y, g_b_y, g_conv_w, g_conv_b, g_w_a, g_b_a, g_w_i, g_b_i, g_a_param, g_w_out, g_b_out)


def solution(mesh):
    cp_size = mesh.shape["cp"]
    fwd_perm = [(j, j + 1) for j in range(cp_size - 1)]
    back_perm = [(j + 1, j) for j in range(cp_size - 1)]

    def per_device(*args):
        return shard_body(*args, fwd_perm=fwd_perm, back_perm=back_perm, cp_size=cp_size, tp_size=mesh.shape["tp"])

    return jax.shard_map(per_device, mesh=mesh, in_specs=IN_SPECS, out_specs=OUT_SPECS, check_vma=False)
```

```python
import functools
import jax
import jax.numpy as jnp
from jax import lax
from jax.experimental import pallas as pl
from jax.experimental.pallas import tpu as pltpu
from jax.sharding import PartitionSpec as P

NORM_EPS = 1e-6
CONV_WIDTH = 4
HALO = CONV_WIDTH - 1
LANES = 128
CB = 256
TC = 16
TINY = 1.2e-38
GELU_A = 0.7978845608028654
GELU_B = 0.044715
VMEM_BYTES = 67043328
F32 = jnp.float32
BF16 = jnp.bfloat16
TOKENS, COLS, CHANNEL = P(None, "cp"), P(None, "tp"), P("tp")
PARAM_SPECS = (P(), COLS, CHANNEL, COLS, CHANNEL, COLS, CHANNEL, CHANNEL, CHANNEL, CHANNEL, CHANNEL, CHANNEL, CHANNEL, P())
IN_SPECS = (TOKENS, TOKENS, TOKENS, *PARAM_SPECS)
OUT_SPECS = (TOKENS, TOKENS, *PARAM_SPECS)
R_BX, R_BY, R_CB, R_BA, R_BI, R_K, R_CW = range(7)
PAR_ROWS = 16
EXT_ROWS = 48
EXT_PAR = 256
N_TILE = 512
SUB = 8
B_BLK = 16


def dot_nn(lhs, rhs):
    return jnp.dot(lhs, rhs, preferred_element_type=F32)


def dot_nt(lhs, rhs):
    return lax.dot_general(lhs, rhs, (((1,), (1,)), ((), ())), preferred_element_type=F32)


def dot_tn(lhs, rhs):
    return lax.dot_general(lhs, rhs, (((0,), (0,)), ((), ())), preferred_element_type=F32)


def round16(val):
    return val.astype(BF16).astype(F32)


def sigmoid(val):
    return 1.0 / (1.0 + jnp.exp(-val))


def gates(pre_a, pre_i, slope, keep):
    gate_r = sigmoid(pre_a)
    gate_i = sigmoid(pre_i)
    log_a = gate_r * slope
    raw_a = jnp.exp(log_a)
    gap = jnp.tanh(-log_a) * (1.0 + raw_a * raw_a)
    inv_m = lax.rsqrt(jnp.maximum(gap, TINY))
    decay = jnp.where(keep, raw_a, 0.0)
    mult = jnp.where(keep, gap * inv_m, 1.0)
    return gate_r, gate_i, decay, mult, inv_m


def first_pass_kernel(n_ref, gz_ref, nh_ref, pos_ref, *rest, n_blk, n_chunk, own, unroll, batch):
    if own:
        ext, rest = rest[0], rest[1:]
        w_hbm, rest = rest[:3], rest[3:]
        c_out, y_out, g_out, q_out, info_out, xb_out, xh, w16, wo16, w_sem, xs, ys, ds, pre, tail, state = rest
    else:
        w_hbm, rest = rest[:4 * n_blk], rest[4 * n_blk:]
        c_out, y_out, g_out, q_out, info_out, ext, w_out, w16, stage, w_sem, o_sem, xs, ys, ds, pre, xh, tail, state = rest
        xb_out = None
    step = pl.program_id(0)
    width = n_ref.shape[1]
    quarter = width // 4

    def own_loads(blk):
        cols = pl.ds(blk * CB, CB)
        pair = [pltpu.make_async_copy(w_hbm[k].at[:, cols], w16.at[blk, k], w_sem.at[blk, k]) for k in range(2)]
        return pair + [pltpu.make_async_copy(w_hbm[2].at[cols, :], wo16.at[blk], w_sem.at[blk, 2])]

    def far_load(idx):
        return pltpu.make_async_copy(w_hbm[idx], stage.at[idx % 4], w_sem.at[idx])

    def stores(blk):
        return [pltpu.make_async_copy(w16.at[blk, k], w_out.at[k, :, pl.ds(blk * CB, CB)], o_sem.at[blk, k]) for k in range(3)]

    def dots(blk):
        rows = n_ref[:]
        xs[blk] = dot_nn(rows, w16[blk, 0])
        ys[blk] = dot_nn(rows, w16[blk, 1])
        ds[blk] = dot_nt(gz_ref[:], wo16[blk]) if own else dot_nn(gz_ref[:], w16[blk, 2])

    def fetch(blk):
        if own:
            for copy in own_loads(blk):
                copy.wait()
        else:
            core = lax.rem(lax.axis_index("cp"), 2)
            for i in range(4):
                far_load(4 * blk + i).wait()
                side = core if i < 2 else 1 - core
                start = pl.multiple_of((2 * side + i % 2) * quarter, quarter)
                for k in range(3):
                    w16[blk, k, pl.ds(start, quarter), :] = stage[i, k, :quarter].astype(BF16)
                    if i < 2:
                        ext[blk, (3 * i + k) * EXT_ROWS:(3 * i + k + 1) * EXT_ROWS] = stage[i, k, quarter:]
                if blk + 1 < n_blk:
                    far_load(4 * blk + 4 + i).start()
            for copy in stores(blk):
                copy.start()
        xh[blk] = dot_nn(nh_ref[:].astype(BF16), w16[blk, 0])

    def elementwise(blk):
        first = step == 1
        for half in range(CB // LANES):
            lane = slice(half * LANES, (half + 1) * LANES)
            row = lambda idx: ext[blk, EXT_PAR + idx:EXT_PAR + idx + 1, lane]
            bias_x, conv_b = row(R_BX), row(R_CB)
            taps = [row(R_CW + k) for k in range(CONV_WIDTH)]
            past = []
            for j in range(HALO):
                sl = slice(j * batch, (j + 1) * batch)
                past.append(jnp.where(first, round16(xh[blk, sl, lane] + bias_x), tail[blk, sl, lane]))
            for t in range(TC):
                sl = slice(t * batch, (t + 1) * batch)
                cur = round16(xs[blk, sl, lane] + bias_x)
                if own:
                    xb_out[blk, t, :, lane] = cur.astype(BF16)
                pos = pos_ref[t]
                total = conv_b + cur * taps[0]
                for k in range(1, CONV_WIDTH):
                    total = total + jnp.where(pos >= k, past[HALO - k], 0.0) * taps[k]
                c_out[blk, t, :, lane] = total.astype(BF16)
                past = past[1:] + [cur]
            for j in range(HALO):
                tail[blk, j * batch:(j + 1) * batch, lane] = past[j]
            wg = ext[blk, half * LANES:(half + 1) * LANES].astype(BF16)
            pre[half] = dot_nn(c_out[blk, :, :, lane].reshape(TC * batch, LANES), wg)
            bias_y, bias_a, bias_i, slope = row(R_BY), row(R_BA), row(R_BI), row(R_K)
            hid = jnp.where(first, 0.0, state[blk, 0, :, lane])
            prod = jnp.where(first, 1.0, state[blk, 1, :, lane])
            head = jnp.where(first, 0.0, state[blk, 2, :, lane])
            for t in range(TC):
                sl = slice(t * batch, (t + 1) * batch)
                keep = pos_ref[t] >= 1
                conv = c_out[blk, t, :, lane].astype(F32)
                _, gate_i, decay, mult, _ = gates(pre[half, sl, :LANES] + bias_a, pre[half, sl, LANES:] + bias_i, slope, keep)
                hid = decay * hid + mult * gate_i * conv
                prod = prod * decay
                pre_y = ys[blk, sl, lane] + bias_y
                sq = pre_y * pre_y
                tan = jnp.tanh(pre_y * (GELU_A + GELU_A * GELU_B * sq))
                half_y = 0.5 * pre_y
                d_mixed = ds[blk, sl, lane]
                y_act = half_y + half_y * tan
                slope_y = 0.5 + 0.5 * tan + half_y * (1.0 - tan * tan) * (GELU_A + 3.0 * GELU_A * GELU_B * sq)
                grad_h = d_mixed * y_act
                head = head + prod * grad_h
                y_out[blk, t, :, lane] = y_act
                g_out[blk, t, :, lane] = grad_h
                q_out[blk, t, :, lane] = d_mixed * slope_y
            for idx, val in enumerate((hid, prod, head)):
                state[blk, idx, :, lane] = val
                info_out[blk, idx, :, lane] = val

    @pl.when(step == 0)
    def _():
        if own:
            for blk in range(n_blk):
                for copy in own_loads(blk):
                    copy.start()
        else:
            for i in range(4):
                far_load(i).start()
        for blk in range(n_blk):
            fetch(blk)
            dots(blk)

    @pl.when((step > 0) & (step < n_chunk))
    def _():
        def both(blk, _):
            elementwise(blk)
            dots(blk)
            return 0

        if unroll:
            for blk in range(n_blk):
                both(blk, 0)
        else:
            lax.fori_loop(0, n_blk, both, 0)

    @pl.when(step == n_chunk)
    def _():
        def last(blk, _):
            elementwise(blk)
            return 0

        lax.fori_loop(0, n_blk, last, 0)
        if not own:
            for blk in range(n_blk):
                for copy in stores(blk):
                    copy.wait()


def first_pass(n_blk, normed, gz, n_halo, pos_b, weights, ext=None, unroll=True):
    own = ext is not None
    n_rows, width = normed.shape
    n_tok, batch = pos_b.shape[0], pos_b.shape[1]
    n_chunk = n_tok // TC
    cols = n_blk * CB
    rows = TC * batch
    cur = lambda s: jnp.minimum(s, n_chunk - 1)
    old = lambda s: jnp.maximum(s - 1, 0)
    const = lambda shape: pl.BlockSpec(shape, lambda s: (0,) * len(shape))
    row_spec = pl.BlockSpec((rows, width), lambda s: (cur(s), 0))
    any_spec = pl.BlockSpec(memory_space=pl.ANY)
    in_specs = [row_spec, row_spec, const((HALO * batch, width)), pl.BlockSpec((TC, batch, LANES), lambda s: (old(s), 0, 0))]
    tok_spec = pl.BlockSpec((n_blk, TC, batch, CB), lambda s: (0, old(s), 0, 0))
    tok_shape = lambda dt: jax.ShapeDtypeStruct((n_blk, n_tok, batch, CB), dt)
    ext_shape = (n_blk, 6 * EXT_ROWS, CB)
    out_specs = [tok_spec] * 4 + [const((n_blk, 3, batch, CB))]
    out_shape = [tok_shape(BF16), tok_shape(F32), tok_shape(F32), tok_shape(F32), jax.ShapeDtypeStruct((n_blk, 3, batch, CB), F32)]
    work = [pltpu.VMEM((n_blk, rows, CB), F32)] * 3 + [pltpu.VMEM((CB // LANES, rows, 2 * LANES), F32)]
    halo = pltpu.VMEM((n_blk, HALO * batch, CB), F32)
    state = pltpu.VMEM((n_blk, 3, batch, CB), F32)
    args = [normed, gz, n_halo, pos_b]
    if own:
        in_specs.append(const(ext_shape))
        args.append(ext)
        out_specs += [tok_spec, const((n_blk, HALO * batch, CB))]
        out_shape += [tok_shape(BF16), jax.ShapeDtypeStruct((n_blk, HALO * batch, CB), F32)]
        scratch = [pltpu.VMEM((n_blk, 2, width, CB), BF16), pltpu.VMEM((n_blk, CB, width), BF16), pltpu.SemaphoreType.DMA((n_blk, 3)), *work, halo, state]
    else:
        out_specs += [const(ext_shape), any_spec]
        out_shape += [jax.ShapeDtypeStruct(ext_shape, F32), jax.ShapeDtypeStruct((3, width, cols), BF16)]
        scratch = [pltpu.VMEM((n_blk, 3, width, CB), BF16), pltpu.VMEM((4, *weights[0].shape), F32), pltpu.SemaphoreType.DMA((4 * n_blk,)), pltpu.SemaphoreType.DMA((n_blk, 3)), *work, halo, halo, state]
    in_specs += [any_spec] * len(weights)
    flops = 6 * n_rows * width * cols
    return pl.pallas_call(
        functools.partial(first_pass_kernel, n_blk=n_blk, n_chunk=n_chunk, own=own, unroll=unroll, batch=batch),
        grid=(n_chunk + 1,), in_specs=in_specs, out_specs=out_specs, scratch_shapes=scratch, out_shape=out_shape,
        compiler_params=pltpu.CompilerParams(dimension_semantics=("arbitrary",), vmem_limit_bytes=VMEM_BYTES),
        cost_estimate=pl.CostEstimate(flops=flops, bytes_accessed=n_rows * width * 4, transcendentals=0),
        name="first_pass_own" if own else "first_pass_far",
    )(*args, *weights)


def turned(val):
    return jnp.swapaxes(val, 0, 1)


def lane_tiles(width):
    return [slice(k, k + LANES) for k in range(0, width, LANES)]


def pre_kernel(x_ref, gz_ref, s_ref, n_out, gz_out, inv_out, gb_out):
    width = x_ref.shape[2]
    total = 0.0
    for lane in lane_tiles(width):
        x_f = x_ref[:, :, lane].astype(F32)
        total = total + x_f * x_f
    inv_out[:] = jnp.broadcast_to(lax.rsqrt(jnp.sum(total, axis=-1, keepdims=True) * (1.0 / width) + NORM_EPS), inv_out.shape)

    @pl.when(pl.program_id(0) == 0)
    def _():
        gb_out[:] = jnp.zeros_like(gb_out)

    for lane in lane_tiles(width):
        normed = x_ref[:, :, lane].astype(F32) * inv_out[:] * (1.0 + s_ref[:, lane])
        n_out[:, :, lane] = turned(normed).astype(BF16)
        gz_f = gz_ref[:, :, lane].astype(F32)
        gz_out[:, :, lane] = turned(gz_f).astype(BF16)
        gb_out[:, lane] += jnp.sum(gz_f.reshape(-1, SUB, LANES), axis=0)


def row_specs(batch, n_tok, b_blk=B_BLK):
    per = batch // b_blk
    n_steps = (n_tok // TC) * per
    cur = lambda s: jnp.minimum(s, n_steps - 1)
    old = lambda s: jnp.maximum(s - 1, 0)
    act = lambda lanes: pl.BlockSpec((TC, b_blk, lanes), lambda s: (cur(s) // per, lax.rem(cur(s), per), 0))
    native = lambda lag, lanes: pl.BlockSpec((b_blk, TC, lanes), lambda s: (lax.rem(lag(s), per), lag(s) // per, 0))
    return n_steps, cur, old, act, native


def pre_pass(x_in, grad_z, scale):
    batch, n_tok, width = x_in.shape
    n_steps, cur, _, act, native = row_specs(batch, n_tok, batch)
    const = lambda shape: pl.BlockSpec(shape, lambda s: (0,) * len(shape))
    return pl.pallas_call(
        pre_kernel, grid=(n_steps,),
        in_specs=[native(cur, width), native(cur, width), const((1, width))], out_specs=[act(width), act(width), native(cur, LANES), const((SUB, width))],
        out_shape=[jax.ShapeDtypeStruct((n_tok, batch, width), BF16)] * 2 + [jax.ShapeDtypeStruct((batch, n_tok, LANES), F32), jax.ShapeDtypeStruct((SUB, width), F32)],
        compiler_params=pltpu.CompilerParams(dimension_semantics=("arbitrary",), vmem_limit_bytes=VMEM_BYTES),
        cost_estimate=pl.CostEstimate(flops=n_tok * batch * width * 200, bytes_accessed=n_tok * batch * width * 8, transcendentals=0),
        name="pre_pass",
    )(x_in, grad_z, scale)


def send_kernel(core_ref, wx_ref, wy_ref, wo_ref, ext_ref, *outs):
    quarter = wx_ref.shape[0]
    for idx, out in enumerate(outs):
        @pl.when(pl.program_id(0) == idx)
        def _():
            values = wx_ref[:].astype(F32), wy_ref[:].astype(F32), wo_ref[:].astype(F32).T
            for k, val in enumerate(values):
                out[k, :quarter] = val
                out[k, quarter:] = ext_ref[0, k * EXT_ROWS:(k + 1) * EXT_ROWS]


def send_pass(core, w_x, w_y, w_out, ext):
    (width, _), n_own = w_x.shape, len(ext)
    quarter = width // 4
    tall = pl.BlockSpec((quarter, CB), lambda i, core: (2 * core[0] + lax.rem(i, 2), i // 2))
    wide = pl.BlockSpec((CB, quarter), lambda i, core: (i // 2, 2 * core[0] + lax.rem(i, 2)))
    shape = (3, quarter + EXT_ROWS, CB)
    return pl.pallas_call(
        send_kernel,
        grid_spec=pltpu.PrefetchScalarGridSpec(num_scalar_prefetch=1, grid=(2 * n_own,), in_specs=[tall, tall, wide, pl.BlockSpec((1, 3 * EXT_ROWS, CB), lambda i, core: (i // 2, lax.rem(i, 2), 0))],
                                               out_specs=[pl.BlockSpec(shape, lambda i, core: (0, 0, 0))] * (2 * n_own)),
        out_shape=[jax.ShapeDtypeStruct(shape, F32)] * (2 * n_own),
        compiler_params=pltpu.CompilerParams(dimension_semantics=("arbitrary",), vmem_limit_bytes=VMEM_BYTES),
        cost_estimate=pl.CostEstimate(flops=10 ** 9, bytes_accessed=2 * 10 ** 7, transcendentals=0),
        name="send_pass",
    )(core, w_x, w_y, w_out, ext)


N_ACC = 10
ACC_ROWS = 8 * N_ACC


def second_pass_kernel(c_ref, y_ref, g_ref, q_ref, pos_ref, enter_ref, wg_ref, par_ref, *rest, n_chunk, own, batch):
    if own:
        xb_ref, xh_ref, mix_out, dpy_out, dbr_out, head_out, tail_out, acc_out, gw_out, s_a, s_A, s_i, s_m, pre, dpai, dgate, s_e = rest
    else:
        mix_out, dpy_out, dbr_out, head_out, tail_out, s_a, s_A, s_i, s_m, pre, dpai, dgate = rest
    row = lambda idx: par_ref[0, idx:idx + 1, :]
    wg = wg_ref[0].astype(BF16)
    enter = (enter_ref[0, 0], enter_ref[0, 1])
    bias_a, bias_i, slope = row(R_BA), row(R_BI), row(R_K)
    taps = [row(R_CW + k) for k in range(CONV_WIDTH)]

    def add(idx, val):
        acc_out[0, pl.ds(8 * idx, 8)] = acc_out[0, pl.ds(8 * idx, 8)] + val

    fold = lambda val: jnp.sum(val.reshape(batch // 8, 8, LANES), axis=0)
    if own:
        halo = [round16(xh_ref[0, k * batch:(k + 1) * batch] + row(R_BX)) for k in range(HALO)]
        acc_out[:] = jnp.zeros_like(acc_out)
        gw_out[:] = jnp.zeros_like(gw_out)

    def chunk_of(j):
        return c_ref[0, pl.ds(j * TC, TC)].reshape(TC * batch, LANES)

    def pre_gates(j):
        pre[:] = dot_nn(chunk_of(j), wg)

    def forward(j, hid):
        base = j * TC
        acc_y = jnp.zeros((8, LANES), F32)
        for t in range(TC):
            sl = slice(t * batch, (t + 1) * batch)
            tok = base + t
            keep = pos_ref[tok] >= 1
            conv = c_ref[0, tok].astype(F32)
            gate_r, gate_i, decay, mult, inv_m = gates(pre[sl, :LANES] + bias_a, pre[sl, LANES:] + bias_i, slope, keep)
            in_conv = gate_i * conv
            before = hid
            hid = decay * before + mult * in_conv
            d_log = decay * (before - in_conv * decay * inv_m)
            r_log = d_log * gate_r
            s_a[tok] = decay
            s_A[tok] = r_log * (1.0 - gate_r) * slope
            s_i[tok] = mult * in_conv * (1.0 - gate_i)
            s_m[tok] = mult * gate_i
            mix_out[tok] = (hid * y_ref[0, tok]).astype(BF16)
            d_pre_y = hid * q_ref[0, tok]
            dpy_out[tok] = d_pre_y.astype(BF16)
            if own:
                s_e[tok] = r_log
                acc_y = acc_y + fold(d_pre_y)
        if own:
            add(1, acc_y)
        pre_gates(jnp.minimum(j + 1, n_chunk - 1))
        return hid

    pre_gates(0)
    lax.fori_loop(0, n_chunk, forward, enter[0], unroll=True)

    def recur(j, carry):
        base = j * TC
        acc_a = acc_i = acc_p = jnp.zeros((8, LANES), F32)
        for t in range(TC - 1, -1, -1):
            sl = slice(t * batch, (t + 1) * batch)
            tok = base + t
            grad_h = g_ref[0, tok] + carry
            carry = s_a[tok] * grad_h
            d_pre_a = grad_h * s_A[tok]
            d_pre_i = grad_h * s_i[tok]
            s_m[tok] = grad_h * s_m[tok]
            dpai[sl, :LANES] = d_pre_a.astype(BF16)
            dpai[sl, LANES:] = d_pre_i.astype(BF16)
            if own:
                acc_a = acc_a + fold(d_pre_a)
                acc_i = acc_i + fold(d_pre_i)
                acc_p = acc_p + fold(grad_h * s_e[tok])
        if own:
            add(2, acc_a)
            add(3, acc_i)
            add(4, acc_p)
            gw_out[0] = gw_out[0] + dot_tn(chunk_of(j), dpai[:])
        return carry

    def conv_back(j, later):
        base = j * TC
        later = list(later)
        acc_x = acc_b = jnp.zeros((8, LANES), F32)
        acc_w = [jnp.zeros((8, LANES), F32) for _ in range(CONV_WIDTH)]
        for t in range(TC - 1, -1, -1):
            sl = slice(t * batch, (t + 1) * batch)
            tok = base + t
            d_conv = s_m[tok] + dgate[sl]
            total = d_conv * taps[0] + later[0]
            pos = pos_ref[tok]
            masked = [jnp.where(pos >= k, d_conv, 0.0) for k in range(1, CONV_WIDTH)]
            later = [later[1] + masked[0] * taps[1], later[2] + masked[1] * taps[2], masked[2] * taps[3]]
            dbr_out[tok] = total.astype(BF16)
            if t >= TC - HALO:
                tail_out[t - (TC - HALO)] = jnp.where(j == n_chunk - 1, total, tail_out[t - (TC - HALO)])
            if own:
                acc_x = acc_x + fold(total)
                acc_b = acc_b + fold(d_conv)
                acc_w[0] = acc_w[0] + fold(d_conv * xb_ref[0, tok].astype(F32))
                for k in range(1, CONV_WIDTH):
                    past = xb_ref[0, jnp.maximum(tok - k, 0)].astype(F32)
                    if t < k:
                        past = jnp.where(j == 0, halo[HALO + t - k], past)
                    acc_w[k] = acc_w[k] + fold(masked[k - 1] * past)
        if own:
            add(0, acc_x)
            add(5, acc_b)
            for k in range(CONV_WIDTH):
                add(6 + k, acc_w[k])
        return tuple(later)

    tail_out[:] = jnp.zeros_like(tail_out)
    zero = jnp.zeros((batch, LANES), F32)
    carry = recur(n_chunk - 1, enter[1])
    dgate[:] = dot_nt(dpai[:], wg)

    def back(idx, vals):
        carry, later = vals[0], vals[1:]
        j = n_chunk - 2 - idx
        carry = recur(j, carry)
        later = conv_back(j + 1, later)
        dgate[:] = dot_nt(dpai[:], wg)
        return (carry, *later)

    vals = lax.fori_loop(0, n_chunk - 1, back, (carry, zero, zero, zero), unroll=True)
    later = conv_back(0, vals[1:])
    for k in range(HALO):
        head_out[HALO - 1 - k] = later[k]


def second_pass(conv, y_act, grad_h, q_val, pos_b, enter, ext, xb=None, xb_halo=None):
    own = xb is not None
    n_blk, n_tok, batch, _ = conv.shape
    n_chunk = n_tok // TC
    per = CB // LANES
    cols = n_blk * CB
    tok_spec = pl.BlockSpec((1, n_tok, batch, LANES), lambda s: (s // per, 0, 0, lax.rem(s, per)))
    lane_spec = lambda n: pl.BlockSpec((n, batch, LANES), lambda s: (0, 0, s))
    in_specs = [tok_spec] * 4 + [pl.BlockSpec((n_tok, batch, LANES), lambda s: (0, 0, 0)),
                pl.BlockSpec((1, 2, batch, LANES), lambda s: (s // per, 0, 0, lax.rem(s, per))),
                pl.BlockSpec((1, LANES, CB), lambda s: (s // per, lax.rem(s, per), 0)),
                pl.BlockSpec((1, PAR_ROWS, LANES), lambda s: (s // per, EXT_PAR // PAR_ROWS, lax.rem(s, per)))]
    out_specs = [lane_spec(n_tok)] * 3 + [lane_spec(HALO)] * 2
    out_shape = [jax.ShapeDtypeStruct((n_tok, batch, cols), BF16)] * 3 + [jax.ShapeDtypeStruct((HALO, batch, cols), F32)] * 2
    scratch = [pltpu.VMEM((n_tok, batch, LANES), F32)] * 4 + [pltpu.VMEM((TC * batch, 2 * LANES), F32), pltpu.VMEM((TC * batch, 2 * LANES), BF16), pltpu.VMEM((TC * batch, LANES), F32)]
    args = [conv, y_act, grad_h, q_val, pos_b, enter, ext, ext]
    if own:
        in_specs += [tok_spec, pl.BlockSpec((1, HALO * batch, LANES), lambda s: (s // per, 0, lax.rem(s, per)))]
        out_specs += [pl.BlockSpec((1, ACC_ROWS, LANES), lambda s: (s, 0, 0)), pl.BlockSpec((1, LANES, 2 * LANES), lambda s: (s, 0, 0))]
        out_shape += [jax.ShapeDtypeStruct((n_blk * per, ACC_ROWS, LANES), F32), jax.ShapeDtypeStruct((n_blk * per, LANES, 2 * LANES), F32)]
        scratch.append(pltpu.VMEM((n_tok, batch, LANES), F32))
        args += [xb, xb_halo]
    n_elem = n_tok * batch * cols
    return pl.pallas_call(
        functools.partial(second_pass_kernel, n_chunk=n_chunk, own=own, batch=batch),
        grid=(n_blk * per,), in_specs=in_specs, out_specs=out_specs, scratch_shapes=scratch, out_shape=out_shape,
        compiler_params=pltpu.CompilerParams(dimension_semantics=("arbitrary",), vmem_limit_bytes=VMEM_BYTES),
        cost_estimate=pl.CostEstimate(flops=n_elem * 12000, bytes_accessed=n_elem * 20, transcendentals=n_elem * 6),
        name="second_pass_own" if own else "second_pass_far",
    )(*args)


def tile_of(j):
    return pl.ds(pl.multiple_of(j * N_TILE, N_TILE), N_TILE)


def out_kernel(*refs, n_part, n_steps, n_pass):
    mixes, refs = refs[:n_part], refs[n_part:]
    w_hbm, refs = refs[:n_part], refs[n_part:]
    pass_in, refs = refs[:n_pass], refs[n_pass:]
    x_ref, b_ref, z_ref, refs = refs[0], refs[1], refs[2], refs[3:]
    pass_out, refs = refs[:n_pass], refs[n_pass:]
    w_v, acc, sem = refs[:n_part], refs[n_part], refs[n_part + 1]
    rows = TC * B_BLK
    n_tiles = z_ref.shape[2] // N_TILE
    step = pl.program_id(0)

    def copies(j):
        tile = tile_of(j)
        first = pltpu.make_async_copy(w_hbm[0].at[:, tile], w_v[0].at[:, tile], sem.at[j, 0])
        return [first] + [pltpu.make_async_copy(w_hbm[i].at[2, tile, :], w_v[i].at[tile, :], sem.at[j, i]) for i in range(1, n_part)]

    def product(tile):
        proj = dot_nn(mixes[0][:].reshape(rows, -1), w_v[0][:, tile])
        for i in range(1, n_part):
            proj = proj + dot_nt(mixes[i][:].reshape(rows, -1), w_v[i][tile, :])
        acc[:, tile] = proj

    def finish():
        for lane in lane_tiles(z_ref.shape[2]):
            proj = turned(acc[:, lane].reshape(TC, B_BLK, LANES))
            z_ref[:, :, lane] = (x_ref[:, :, lane].astype(F32) + (proj + b_ref[:, lane])).astype(BF16)
        for src, dst in zip(pass_in, pass_out):
            dst[:] = src[:]

    @pl.when(step == 0)
    def _():
        for j in range(n_tiles):
            for copy in copies(j):
                copy.start()

        def first(j, _):
            for copy in copies(j):
                copy.wait()
            product(tile_of(j))
            return 0

        lax.fori_loop(0, n_tiles, first, 0)

    @pl.when((step > 0) & (step < n_steps))
    def _():
        finish()
        product(slice(None))

    @pl.when(step == n_steps)
    def _():
        finish()


def out_pass(mixes, w_own, w_far, x_in, b_out, sums):
    n_tok, batch, _ = mixes[0].shape
    width = x_in.shape[2]
    n_steps, _, old, act, native = row_specs(batch, n_tok)
    n_part = len(mixes)
    any_spec = pl.BlockSpec(memory_space=pl.ANY)
    strips = [pl.BlockSpec((g.shape[0] // n_steps, g.shape[1]), lambda s: (old(s), 0)) for g in sums]
    return pl.pallas_call(
        functools.partial(out_kernel, n_part=n_part, n_steps=n_steps, n_pass=len(sums)), grid=(n_steps + 1,),
        in_specs=[act(m.shape[2]) for m in mixes] + [any_spec] * n_part + strips + [native(old, width), pl.BlockSpec((1, width), lambda s: (0, 0))],
        out_specs=[native(old, width)] + strips, out_shape=[jax.ShapeDtypeStruct(a.shape, a.dtype) for a in (x_in, *sums)],
        scratch_shapes=[pltpu.VMEM(w_own.shape, BF16)] + [pltpu.VMEM(w.shape[1:], BF16) for w in w_far] + [pltpu.VMEM((TC * B_BLK, width), F32), pltpu.SemaphoreType.DMA((width // N_TILE, n_part))],
        compiler_params=pltpu.CompilerParams(dimension_semantics=("arbitrary",), vmem_limit_bytes=VMEM_BYTES),
        cost_estimate=pl.CostEstimate(flops=2 * n_tok * batch * width * width, bytes_accessed=n_tok * batch * width * 8, transcendentals=0),
        name="out_pass",
    )(*mixes, w_own, *w_far, *sums, x_in, b_out)


def norm_back_kernel(*refs, n_part, n_steps):
    n_all = 2 * n_part
    lhs, refs = refs[:n_all], refs[n_all:]
    w_hbm, refs = refs[:n_part + 1], refs[n_part + 1:]
    x_ref, inv_ref, gz_ref, s_ref, gx_ref, gs_ref, *refs = refs
    w_v, (acc, d_n, x_old, sums, scale, shift, sem) = refs[:n_all], refs[n_all:]
    rows = TC * B_BLK
    width = gx_ref.shape[2]
    n_tiles = width // N_TILE
    wide = width // 2
    step = pl.program_id(0)

    def copies(j):
        tile = tile_of(j)
        lst = []
        for k in range(2):
            for i in range(n_part):
                src = w_hbm[k].at[tile, :] if i == 0 else w_hbm[i + 1].at[k, tile, :]
                idx = k * n_part + i
                lst.append(pltpu.make_async_copy(src, w_v[idx].at[tile, :], sem.at[j, idx]))
        return lst

    def product(tile):
        val = dot_nt(lhs[0][:].reshape(rows, -1), w_v[0][tile, :])
        for arr, weight in zip(lhs[1:], w_v[1:]):
            val = val + dot_nt(arr[:].reshape(rows, -1), weight[tile, :])
        acc[:, tile] = val

    def turn(tiles):
        for lane in tiles:
            val = turned(acc[:, lane].reshape(TC, B_BLK, LANES))
            d_n[:, :, lane] = val
            x_t = x_ref[:, :, lane]
            x_old[:, :, lane] = x_t
            sums[:] += val * (1.0 + s_ref[:, lane]) * x_t.astype(F32)

    def close():
        inv = inv_ref[:]
        scale[:] = inv
        shift[:] = inv * inv * inv * (jnp.sum(sums[:], axis=-1, keepdims=True) * (1.0 / width))
        sums[:] = jnp.zeros_like(sums)

    def finish():
        for lane in lane_tiles(width):
            val, inv = d_n[:, :, lane], scale[:]
            x_f = x_old[:, :, lane].astype(F32)
            gx_ref[:, :, lane] = (gz_ref[:, :, lane].astype(F32) + (inv * (val * (1.0 + s_ref[:, lane])) - x_f * shift[:])).astype(BF16)
            gs_ref[:, lane] += jnp.sum((val * x_f * inv).reshape(-1, SUB, LANES), axis=0)

    low, high = lane_tiles(width)[:wide // LANES], lane_tiles(width)[wide // LANES:]

    @pl.when(step == 0)
    def _():
        gs_ref[:] = jnp.zeros_like(gs_ref)
        sums[:] = jnp.zeros_like(sums)
        for j in range(n_tiles):
            for copy in copies(j):
                copy.start()

        def first(j, _):
            for copy in copies(j):
                copy.wait()
            product(tile_of(j))
            return 0

        lax.fori_loop(0, n_tiles, first, 0)
        turn(low + high)
        close()

    @pl.when((step > 0) & (step < n_steps))
    def _():
        finish()
        product(slice(wide))
        turn(low)
        product(slice(wide, None))
        turn(high)
        close()

    @pl.when(step == n_steps)
    def _():
        finish()


def norm_back_pass(dbrs, dpys, wx_own, wy_own, w_far, x_in, inv_b, grad_z, scale):
    n_tok, batch, _ = dbrs[0].shape
    width = x_in.shape[2]
    n_steps, cur, old, act, native = row_specs(batch, n_tok)
    n_part = len(dbrs)
    const = lambda shape: pl.BlockSpec(shape, lambda s: (0,) * len(shape))
    planes = [pltpu.VMEM(wx_own.shape, BF16)] + [pltpu.VMEM(w.shape[1:], BF16) for w in w_far]
    block = lambda dt, lanes: pltpu.VMEM((B_BLK, TC, lanes), dt)
    return pl.pallas_call(
        functools.partial(norm_back_kernel, n_part=n_part, n_steps=n_steps), grid=(n_steps + 1,),
        in_specs=[act(m.shape[2]) for m in (*dbrs, *dpys)] + [pl.BlockSpec(memory_space=pl.ANY)] * (n_part + 1) + [native(cur, width), native(cur, LANES), native(old, width), const((1, width))],
        out_specs=[native(old, width), const((SUB, width))],
        out_shape=[jax.ShapeDtypeStruct(x_in.shape, BF16), jax.ShapeDtypeStruct((SUB, width), F32)],
        scratch_shapes=[*planes, *planes, pltpu.VMEM((TC * B_BLK, width), F32), block(F32, width), block(BF16, width), *[block(F32, LANES)] * 3, pltpu.SemaphoreType.DMA((width // N_TILE, 2 * n_part))],
        compiler_params=pltpu.CompilerParams(dimension_semantics=("arbitrary",), vmem_limit_bytes=VMEM_BYTES),
        cost_estimate=pl.CostEstimate(flops=4 * n_tok * batch * width * width, bytes_accessed=n_tok * batch * width * 10, transcendentals=0),
        name="norm_back_pass",
    )(*dbrs, *dpys, wx_own, wy_own, *w_far, x_in, inv_b, grad_z, scale)


def after(val, *deps):
    return lax.optimization_barrier((val, *deps))[0]


def entering(info, cp_index, swap_core, swap_x):
    end, prod, head = [info[:, k] for k in range(3)]
    other = lax.ppermute(info, "cp", swap_core)
    o_end, o_prod, o_head = [other[:, k] for k in range(3)]
    upper_core = cp_index % 2 == 1
    upper_chip = cp_index >= 2
    chip_end = jnp.where(upper_core, prod * o_end + end, o_prod * end + o_end)
    chip_head = jnp.where(upper_core, o_head + o_prod * head, head + prod * o_head)
    got = lax.ppermute(jnp.where(upper_chip, chip_head, chip_end), "cp", swap_x)
    from_low = jnp.where(upper_chip, got, 0.0)
    from_high = jnp.where(upper_chip, 0.0, got)
    state_in = jnp.where(upper_core, o_prod * from_low + o_end, from_low)
    grad_in = jnp.where(upper_core, from_high, o_head + o_prod * from_high)
    return jnp.stack([state_in, grad_in], axis=1)


def shard_body(x_in, grad_z, seg_pos, norm_scale, w_x, b_x, w_y, b_y, conv_w, conv_b, w_a, b_a, w_i, b_i, a_param, w_out, b_out, fwd_perm, back_perm, cp_size, tp_size):
    cp_index = lax.axis_index("cp")
    batch, n_tok, width = x_in.shape
    c_own = w_x.shape[1]
    n_own = c_own // CB
    swap_core = [(j, j ^ 1) for j in range(cp_size)]
    swap_x = [(j, j ^ 2) for j in range(cp_size)]

    slope = -8.0 * jax.nn.softplus(a_param)
    rows = [b_x, b_y, conv_b, b_a, b_i, slope, *[conv_w[k] for k in range(CONV_WIDTH)]]
    par = jnp.stack([r.astype(F32) for r in rows] + [jnp.zeros_like(slope)] * (PAR_ROWS - len(rows)))
    par = par.reshape(PAR_ROWS, n_own, CB).transpose(1, 0, 2)
    wg = jnp.concatenate([w_a, w_i], axis=-1).astype(F32).reshape(n_own, EXT_PAR, CB)
    ext = jnp.concatenate([wg, par, jnp.zeros((n_own, 6 * EXT_ROWS - EXT_PAR - PAR_ROWS, CB), F32)], axis=1)

    x_halo = lax.ppermute(x_in[:, n_tok - HALO:].astype(F32).transpose(1, 0, 2), "cp", fwd_perm)
    core = jnp.full((1,), cp_index % 2, jnp.int32)
    mine = send_pass(core, w_x, w_y, w_out, ext)
    to_y, to_z = [[(k, k ^ m) for k in range(tp_size)] for m in (1, 2)]
    got = {}
    for p in range(n_own):
        for u in range(2):
            got["y", p, u] = lax.ppermute(mine[2 * p + u], "tp", to_y)
            got["z", p, u] = lax.ppermute(mine[2 * p + u], "tp", to_z)
    for p in range(n_own):
        got["d", p, 0] = lax.ppermute(got["y", p, 0], "tp", to_z)
        got["d", p, 1] = lax.ppermute(got["z", p, 1], "tp", to_y)

    def blocks(keys):
        lst = []
        for way, p in keys:
            pair = [got[way, p, u] for u in range(2)]
            lst += pair
            for arr in pair:
                lst.append(lax.ppermute(arr, "cp", swap_core))
        return lst

    normed, gz_t, inv_b, gb_part = pre_pass(after(x_in, *mine), grad_z, norm_scale.astype(F32).reshape(1, width))
    inv_h = lax.rsqrt(jnp.mean(x_halo * x_halo, axis=-1, keepdims=True) + NORM_EPS)
    n_halo = (x_halo * inv_h * (1.0 + norm_scale.astype(F32))).reshape(HALO * batch, width)
    normed = normed.reshape(n_tok * batch, width)
    gz_t = gz_t.reshape(n_tok * batch, width)
    pos_b = jnp.broadcast_to(seg_pos.T[:, :, None], (n_tok, batch, LANES))
    flat = lambda arr: arr.reshape(n_tok * batch, -1)

    c_o, y_o, g_o, q_o, info_o, xb_o, xh_o = first_pass(n_own, normed, gz_t, n_halo, pos_b, [w_x, w_y, w_out], ext)
    enter_o = entering(info_o, cp_index, swap_core, swap_x)
    mix_o, dpy_o, dbr_o, head_o, tail_o, acc, g_gate = second_pass(c_o, y_o, g_o, q_o, pos_b, enter_o, ext, xb_o, xh_o)
    back_o = lax.ppermute(head_o, "cp", back_perm)
    dbr_o = dbr_o.at[n_tok - HALO:].set((tail_o + back_o).astype(BF16))
    g_w_out = dot_tn(flat(mix_o), gz_t)
    g_w_y = dot_tn(normed, flat(dpy_o))
    g_w_x = dot_tn(after(normed, g_w_y, g_w_out), flat(dbr_o))

    calls = [[("y", 0), ("z", 0), ("y", 1)], [("z", 1), ("y", 2), ("z", 2)], [("d", 0), ("d", 1), ("d", 2)]]
    mixes, dpys, dbrs, w_far = [mix_o], [dpy_o], [dbr_o], []
    firsts = {}
    last = g_w_x
    for kind, idx in (("first", 0), ("second", 0), ("first", 1), ("first", 2), ("second", 1), ("second", 2)):
        if kind == "first":
            rows_n = after(normed, last)
            arrays = blocks(calls[idx])
            *acts, last, ext_f, w16 = first_pass(len(calls[idx]), rows_n, gz_t, n_halo, pos_b, arrays, unroll=idx == len(calls) - 1)
            firsts[idx] = acts, entering(last, cp_index, swap_core, swap_x), ext_f
            w_far.append(w16)
            continue
        (conv, *acts), enter_f, ext_f = firsts[idx]
        conv = after(conv, last)
        last, dpy_f, dbr_f, head_f, tail_f = second_pass(conv, *acts, pos_b, enter_f, ext_f)
        back_f = lax.ppermute(head_f, "cp", back_perm)
        dbr_f = dbr_f.at[n_tok - HALO:].set((tail_f + back_f).astype(BF16))
        for lst, val in zip((mixes, dpys, dbrs), (last, dpy_f, dbr_f)):
            lst.append(val)
    grad_x, gs_part = norm_back_pass(dbrs, dpys, w_x, w_y, w_far, x_in, inv_b, grad_z, norm_scale.astype(F32).reshape(1, width))
    acc = acc.reshape(c_own // LANES, N_ACC, 8, LANES).sum(axis=2).transpose(1, 0, 2).reshape(N_ACC, c_own)
    g_b_x = acc[:1] + jnp.sum(back_o, axis=(0, 1))
    g_a_param = -8.0 * jax.nn.sigmoid(a_param) * acc[4:5]
    g_b_out = jnp.sum(gb_part, axis=0).reshape(-1, c_own)
    smalls = jnp.concatenate([g_b_x, acc[1:4], g_a_param, acc[5:], g_b_out])
    n_small = smalls.shape[0]
    packed = jnp.concatenate([g_gate.reshape(-1, CB), jnp.pad(smalls, ((0, PAR_ROWS - n_small), (0, 0))).reshape(-1, CB)])
    g_w_x, g_w_y, g_w_out, packed = lax.psum((g_w_x, g_w_y, g_w_out, packed), "cp")
    g_gate = packed[:c_own].reshape(g_gate.shape)
    g_w_a, g_w_i = g_gate[:, :, :LANES], g_gate[:, :, LANES:]
    smalls = packed[c_own:].reshape(PAR_ROWS, c_own)
    g_b_x, g_b_y, g_b_a, g_b_i, g_a_param, g_conv_b = [smalls[k] for k in range(6)]
    g_conv_w, g_b_out = smalls[6:6 + CONV_WIDTH], smalls[6 + CONV_WIDTH:n_small].reshape(-1)
    g_scale = jnp.sum(gs_part, axis=0)
    g_scale = g_scale + sum(lax.ppermute(g_scale, "cp", [(j, j ^ m) for j in range(cp_size)]) for m in range(1, cp_size))
    mixes[0] = after(mixes[0], gs_part)
    z_out, g_w_x, g_w_y, g_w_out = out_pass(mixes, w_out, w_far, x_in, b_out.astype(F32).reshape(1, width), (g_w_x, g_w_y, g_w_out))
    return (z_out, grad_x, g_scale, g_w_x, g_b_x, g_w_y, g_b_y, g_conv_w, g_conv_b, g_w_a, g_b_a, g_w_i, g_b_i, g_a_param, g_w_out, g_b_out)


def solution(mesh):
    cp_size = mesh.shape["cp"]
    fwd_perm = [(j, j + 1) for j in range(cp_size - 1)]
    back_perm = [(j + 1, j) for j in range(cp_size - 1)]

    def per_device(*args):
        return shard_body(*args, fwd_perm=fwd_perm, back_perm=back_perm, cp_size=cp_size, tp_size=mesh.shape["tp"])

    return jax.shard_map(per_device, mesh=mesh, in_specs=IN_SPECS, out_specs=OUT_SPECS, check_vma=False)
```
